32 devices in a mesh: ta: 8 (over z, x), gx: 4 (over y, core).
Axes of the slice: x: 2, y: 2, z: 4, core: 2. Of those that a mesh axis runs over, the one named last changes fastest.
Arguments:
- links: float32 [16, 4, 18, 32, 512], P('ta', None, None, 'gx'), may hold values from -1 to 1, as said below
Outputs:
- spatial_links: float32 [16, 3, 18, 32, 512], P('ta', None, None, 'gx')
- correlator: float32 [16, 3, 32, 512], P('ta', None, 'gx')
The draws below stay inside these ranges and needn't reach their ends.
Inputs may be any that keep to these rules, and one draw needn't show every extreme that they name: `links`: every link is a special unitary 3 x 3 complex matrix.
All inputs are finite; a program needn't handle non-finite values.
Results may differ from the reference program's by a relative error of at most 0.00023.
Values sent between devices are 32-bit elements; how exact they have to be, the bound alone decides.
No kernel may reach another device: no remote copies, remote signals or barrier semaphores. Data moves between devices by JAX's collectives and lax.ppermute only.
A program may use at most 128 MiB of HBM per device.

```python
import jax
import jax.numpy as jnp
from jax import lax

LZ = 32
NT = 16
LX = 32
LYZ = 512


def subgroup_matrix(alpha, beta, gamma, first, second):
    zero = jnp.zeros_like(alpha)
    one = jnp.ones_like(alpha)
    quat_zero = jnp.cos(alpha)
    quat_three = jnp.sin(alpha) * jnp.cos(beta)
    quat_one = jnp.sin(alpha) * jnp.sin(beta) * jnp.cos(gamma)
    quat_two = jnp.sin(alpha) * jnp.sin(beta) * jnp.sin(gamma)
    real_rows = [[one if i == j else zero for j in range(3)] for i in range(3)]
    imag_rows = [[zero for j in range(3)] for i in range(3)]
    real_rows[first][first] = quat_zero
    imag_rows[first][first] = quat_three
    real_rows[first][second] = quat_two
    imag_rows[first][second] = quat_one
    real_rows[second][first] = -quat_two
    imag_rows[second][first] = quat_one
    real_rows[second][second] = quat_zero
    imag_rows[second][second] = -quat_three
    return (real_rows, imag_rows)


def matrix_product(left, right):
    real_rows = []
    imag_rows = []
    for i in range(3):
        real_line = []
        imag_line = []
        for j in range(3):
            real_sum = 0.0
            imag_sum = 0.0
            for k in range(3):
                real_sum = real_sum + left[0][i][k] * right[0][k][j] - left[1][i][k] * right[1][k][j]
                imag_sum = imag_sum + left[0][i][k] * right[1][k][j] + left[1][i][k] * right[0][k][j]
            real_line.append(real_sum)
            imag_line.append(imag_sum)
        real_rows.append(real_line)
        imag_rows.append(imag_line)
    return (real_rows, imag_rows)


def draw_links(key, part):
    shape = (3, NT, 4, LX, LYZ)
    keys = jax.random.split(jax.random.fold_in(key, 17), 3)
    alpha = jax.random.uniform(keys[0], shape, jnp.float32, 0.0, 3.14159265)
    beta = jax.random.uniform(keys[1], shape, jnp.float32, 0.0, 3.14159265)
    gamma = jax.random.uniform(keys[2], shape, jnp.float32, -3.14159265, 3.14159265)
    pairs = ((0, 1), (1, 2), (0, 2))
    total = subgroup_matrix(alpha[0], beta[0], gamma[0], 0, 1)
    for index in (1, 2):
        factor = subgroup_matrix(alpha[index], beta[index], gamma[index], pairs[index][0], pairs[index][1])
        total = matrix_product(total, factor)
    real_part = jnp.stack([jnp.stack(line) for line in total[0]])
    imag_part = jnp.stack([jnp.stack(line) for line in total[1]])
    matrix = jnp.stack([real_part, imag_part])
    matrix = jnp.transpose(matrix, (3, 4, 0, 1, 2, 5, 6))
    return matrix.reshape((NT, 4, 18, LX, LYZ)).astype(jnp.float32)


def setup_inputs(seed: int = 0) -> dict:
    splits = jax.random.split(jax.random.key(seed), 2)
    links = draw_links(jax.random.fold_in(splits[1], 71), 0)
    return dict(links=links)


def complex_product(left, right):
    real_part = 0.0
    imag_part = 0.0
    for j in range(3):
        lr = left[0][:, j][:, None]
        li = left[1][:, j][:, None]
        rr = right[0][j][None]
        ri = right[1][j][None]
        real_part = real_part + lr * rr - li * ri
        imag_part = imag_part + lr * ri + li * rr
    return jnp.stack([real_part, imag_part])


def dagger(matrix):
    return jnp.stack([jnp.swapaxes(matrix[0], 0, 1), -jnp.swapaxes(matrix[1], 0, 1)])


def identity_field(site_shape):
    eye_real = jnp.broadcast_to(jnp.eye(3, dtype=jnp.float32).reshape((3, 3, 1, 1)), (3, 3) + tuple(site_shape))
    return jnp.stack([eye_real, jnp.zeros_like(eye_real)])


def step_forward(field, direction):
    shape = field.shape
    if direction == 1:
        return jnp.roll(field, -LZ, axis=-1)
    grid = field.reshape(shape[:-1] + (shape[-1] // LZ, LZ))
    return jnp.roll(grid, -1, axis=-1).reshape(shape)


def slice_terms(gauge_ext, links_three, polyakov):
    gauge_own = gauge_ext[..., :-1, :]
    poly_own = polyakov[..., :-1, :]
    results = []
    correlators = []
    for direction in range(3):
        if direction == 0:
            gauge_next = gauge_ext[..., 1:, :]
            poly_next = polyakov[..., 1:, :]
        else:
            gauge_next = step_forward(gauge_own, direction)
            poly_next = step_forward(poly_own, direction)
        moved = complex_product(complex_product(gauge_own, links_three[direction]), dagger(gauge_next))
        left_side = complex_product(poly_own, moved)
        right_side = complex_product(moved, poly_next)
        correlators.append(jnp.sum(left_side * right_side, axis=(0, 1, 2)))
        results.append(moved)
    return jnp.stack(results), jnp.stack(correlators)


def reference(links):
    matrices = links.reshape((NT, 4, 2, 3, 3, LX, LYZ))
    identity = identity_field((LX, LYZ))

    def advance(running, link_matrix):
        return complex_product(running, link_matrix), running

    polyakov, gauge = lax.scan(advance, identity, matrices[:, 3])
    gauge_ext = jnp.concatenate([gauge, gauge[..., :1, :]], axis=-2)
    poly_ext = jnp.concatenate([polyakov, polyakov[..., :1, :]], axis=-2)

    def one_slice(inputs):
        return slice_terms(inputs[0], inputs[1], poly_ext)

    spatial, correlator = lax.map(one_slice, (gauge_ext, matrices[:, :3]))
    return spatial.reshape((NT, 3, 18, LX, LYZ)), correlator
```

```python
import functools

import jax
import jax.numpy as jnp
from jax import lax
from jax.experimental import pallas as pl
from jax.experimental.pallas import tpu as pltpu
from jax.sharding import PartitionSpec as P

LZ = 32
LANES = 128


def total(terms):
    result = terms[0]
    for term in terms[1:]:
        result = result + term
    return result


def dot(left, right):
    pairs = list(zip(left, right))
    real = total([a[0] * b[0] for a, b in pairs]) - total([a[1] * b[1] for a, b in pairs])
    imag = total([a[0] * b[1] for a, b in pairs] + [a[1] * b[0] for a, b in pairs])
    return real, imag


def dot_conj(left, right):
    pairs = list(zip(left, right))
    real = total([a[0] * b[0] for a, b in pairs] + [a[1] * b[1] for a, b in pairs])
    imag = total([a[1] * b[0] for a, b in pairs]) - total([a[0] * b[1] for a, b in pairs])
    return real, imag


def times(rows, matrix):
    columns = [[matrix[k][j] for k in range(3)] for j in range(3)]
    return [[dot(row, column) for column in columns] for row in rows]


def times_dagger(rows, matrix):
    return [[dot_conj(row, other) for other in matrix] for row in rows]


def complete(rows):
    first, second = rows[0], rows[1]
    third = []
    for j in range(3):
        a, b = (j + 1) % 3, (j + 2) % 3
        ar, ai = first[a]
        br, bi = second[b]
        cr, ci = first[b]
        dr, di = second[a]
        third.append((ar * br - ai * bi - cr * dr + ci * di, cr * di + ci * dr - ar * bi - ai * br))
    return [first, second, third]


def pick(flag, yes, no):
    return [
        [(jnp.where(flag, y[0], n[0]), jnp.where(flag, y[1], n[1])) for y, n in zip(yr, nr)]
        for yr, nr in zip(yes, no)
    ]


def unit_rows(like):
    one, zero = jnp.ones_like(like), jnp.zeros_like(like)
    return [[(one if i == j else zero, zero) for j in range(3)] for i in range(2)]


def trace_real(left, right):
    aa = dot_conj(left[0], right[0])
    bb = dot_conj(left[1], right[1])
    ab = dot_conj(left[0], right[1])
    ba = dot_conj(left[1], right[0])
    third = (aa[0] * bb[0] - aa[1] * bb[1]) - (ab[0] * ba[0] - ab[1] * ba[1])
    return aa[0] + bb[0] + third


def matrix_at(at, rows):
    return [[(at(i * 3 + j), at((rows + i) * 3 + j)) for j in range(3)] for i in range(rows)]


def put(at, matrix):
    rows = len(matrix)
    for i in range(rows):
        for j in range(3):
            at(i * 3 + j, matrix[i][j][0])
            at((rows + i) * 3 + j, matrix[i][j][1])


def state_rows(planes, half):
    return 12 * half * (planes + 1)


def groups(planes, half):
    for block in range(half):
        yield lambda k, block=block: pl.ds((k * half + block) * planes, planes)
    for block in range(half):
        yield lambda k, block=block: pl.ds(12 * half * planes + k * half + block, 1)


def take(ref, rows, base=0):
    return matrix_at(lambda k: ref[pl.ds(rows(k).start + base, rows(k).size), :], 2)


def give(ref, rows, matrix, base=0):
    def at(k, value):
        ref[pl.ds(rows(k).start + base, rows(k).size), :] = value
    put(at, matrix)


def bit_of(step):
    return lax.rem(lax.axis_index("ta") // (1 << step), 2)


def lane_block(c):
    return pl.ds(pl.multiple_of(c * LANES, LANES), LANES)


def block_kernel(half, links_ref, keep_ref, send_ref, rim_ref, across_ref):
    slices, _, planes, cells = links_ref.shape
    blocks = cells // LANES
    own = bit_of(0)
    first = lambda m: [[(v[0][:1], v[1][:1]) for v in row] for row in m]
    for which in range(2):
        for block in range(half):
            c = (own if which == 0 else 1 - own) * half + block
            at = lane_block(c)
            link = lambda t: matrix_at(lambda k: links_ref[t, k, :, at], 3)
            rows = link(0)[:2]
            for t in range(1, slices):
                before = first(link(t - 1)[:2])
                base = 12 * half + 12 * blocks * (t - 1)
                def edge(k, value):
                    rim_ref[pl.ds(base + k * blocks + c, 1), :] = value
                put(edge, before)
                rows = times(rows, link(t))
            main = keep_ref if which == 0 else send_ref
            def tile(k, value):
                main[(k * half + block) * planes:(k * half + block + 1) * planes, :] = value
            put(tile, rows)
            side = rim_ref if which == 0 else across_ref
            def row(k, value):
                side[k * half + block:k * half + block + 1, :] = value
            put(row, first(rows))


def pair_kernel(planes, half, keep_ref, seen_ref, rim_ref, across_ref, block_ref, lower_ref):
    upper = bit_of(0) == 1
    tiles = 12 * half * planes
    for index, rows in enumerate(groups(planes, half)):
        if index < half:
            own, seen = take(keep_ref, rows), take(seen_ref, rows)
        else:
            own, seen = take(rim_ref, rows, -tiles), take(across_ref, rows, -tiles)
        low, high = pick(upper, seen, own), pick(upper, own, seen)
        give(block_ref, rows, times(low, complete(high)))
        give(lower_ref, rows, low)


def combine_kernel(planes, half, step, first, last, *refs):
    refs = list(refs)
    block_ref, seen_ref = refs.pop(0), refs.pop(0)
    prefix_ref = None if first else refs.pop(0)
    lower_ref = refs.pop(0) if last else None
    flag = bit_of(step) == 1
    odd = bit_of(0) == 1
    for rows in groups(planes, half):
        own, seen = take(block_ref, rows), take(seen_ref, rows)
        block = times(pick(flag, seen, own), complete(pick(flag, own, seen)))
        if first:
            prefix = pick(flag, seen, unit_rows(seen[0][0][0]))
        else:
            before = take(prefix_ref, rows)
            prefix = pick(flag, times(seen, complete(before)), before)
        give(refs[0], rows, block)
        if last:
            after = times(prefix, complete(take(lower_ref, rows)))
            give(refs[1], rows, pick(odd, after, prefix))
            give(refs[2], rows, block)
            give(refs[2], rows, pick(odd, prefix, after), state_rows(planes, half))
        else:
            give(refs[1], rows, prefix)


def close(flag, block, prefix, seen):
    poly = times(pick(flag, seen, block), complete(pick(flag, block, seen)))
    return poly, pick(flag, times(seen, complete(prefix)), prefix)


def prepare(planes, half, step, other, links_ref, rim_ref, block, prefix, seen, field_ref, edge_ref):
    slices, cells = links_ref.shape[0], links_ref.shape[-1]
    blocks = cells // LANES
    flag = bit_of(step) == 1
    own = bit_of(0)
    for index, rows in enumerate(groups(planes, half)):
        local = index % half
        c = (1 - own if other else own) * half + local
        poly, gauge = close(flag, block(rows), prefix(rows), seen(rows))
        for t in range(slices + 1):
            if 0 < t < slices:
                if index < half:
                    link = matrix_at(lambda k: links_ref[t - 1, 3, k, :, lane_block(c)], 3)
                else:
                    base = 12 * half + 12 * blocks * (t - 1)
                    link = complete(matrix_at(lambda k: rim_ref[pl.ds(base + k * blocks + c, 1), :], 2))
                gauge = times(gauge, link)
            value = complete(gauge if t < slices else poly)
            def store(k, v):
                if index < half:
                    field_ref[local, 18 * t + k] = v
                else:
                    at = (18 * t + k) * half + local
                    edge_ref[at:at + 1, :] = v
            put(store, value)


def shifted(load, direction, r, edge):
    value = load(r)
    lane = lax.broadcasted_iota(jnp.int32, value.shape, 1)
    if direction == 0:
        row = lax.broadcasted_iota(jnp.int32, value.shape, 0)
        mixed = jnp.where(row == 0, jnp.broadcast_to(edge(r), value.shape), value)
        return pltpu.roll(mixed, value.shape[0] - 1, 0)
    if direction == 1:
        mixed = jnp.where(lane < LZ, load(r + 1), value)
        return pltpu.roll(mixed, LANES - LZ, 1)
    ahead = pltpu.roll(value, LANES - 1, 1)
    around = pltpu.roll(value, LZ - 1, 1)
    return jnp.where(lax.rem(lane, LZ) == LZ - 1, around, ahead)


def outputs(half, jobs, links_ref, fields, edges, spatial_ref, correlator_ref, out_ref, trace_ref, sem):
    slices, cells = links_ref.shape[0], links_ref.shape[-1]
    blocks = cells // LANES
    own = bit_of(0)

    def field(r, k):
        r = r % blocks
        return fields[r // half][r % half, k]

    def edge(r, k):
        at = k * half + r % half
        return edges[r // half][at:at + 1, :]

    started = []
    for job, (r, direction) in enumerate(jobs):
        c = lax.rem(own * half + r, blocks)
        at = lane_block(c)

        def neighbour(base):
            def one(k):
                return shifted(lambda q: field(q, base + k), direction, r, lambda q: edge(q, base + k))
            return matrix_at(one, 3)

        poly = matrix_at(lambda k: field(r, 18 * slices + k), 3)[:2]
        poly_next = neighbour(18 * slices)
        for t in range(slices):
            link = matrix_at(lambda k: links_ref[t, direction, k, :, at], 3)
            gauge = matrix_at(lambda k: field(r, 18 * t + k), 3)[:2]
            moved = complete(times_dagger(times(gauge, link), neighbour(18 * t)))
            def store(k, v):
                out_ref[job, t, k] = v
            put(store, moved)
            trace_ref[job, t] = trace_real(times(poly, moved), times(moved[:2], poly_next))
        for copy in (
            pltpu.make_async_copy(out_ref.at[job], spatial_ref.at[:, direction, :, :, at], sem.at[job, 0]),
            pltpu.make_async_copy(trace_ref.at[job], correlator_ref.at[:, direction, :, at], sem.at[job, 1]),
        ):
            copy.start()
            started.append(copy)
    for copy in started:
        copy.wait()


def jobs_of(half, late):
    early = [(r, d) for r in range(half) for d in (0, 2)] + [(r, 1) for r in range(half - 1)]
    rest = [(half - 1, 1)] + [(r, d) for r in range(half, 2 * half) for d in range(3)]
    return rest if late else early


def early_kernel(planes, half, step, links_ref, block_ref, prefix_ref, seen_ref, rim_ref,
                 spatial_ref, correlator_ref, field_ref, edge_ref, out_ref, trace_ref, sem):
    prepare(planes, half, step, False, links_ref, rim_ref, lambda g: take(block_ref, g),
            lambda g: take(prefix_ref, g), lambda g: take(seen_ref, g), field_ref, edge_ref)
    outputs(half, jobs_of(half, False), links_ref, [field_ref, field_ref], [edge_ref, edge_ref],
            spatial_ref, correlator_ref, out_ref, trace_ref, sem)


def late_kernel(planes, half, step, links_ref, pair_ref, seen_ref, rim_ref, field_ref, edge_ref,
                spatial_in, correlator_in, spatial_ref, correlator_ref,
                field_late, edge_late, out_ref, trace_ref, sem):
    size = state_rows(planes, half)
    prepare(planes, half, step, True, links_ref, rim_ref, lambda g: take(pair_ref, g),
            lambda g: take(pair_ref, g, size), lambda g: take(seen_ref, g), field_late, edge_late)
    outputs(half, jobs_of(half, True), links_ref, [field_ref, field_late], [edge_ref, edge_late],
            spatial_ref, correlator_ref, out_ref, trace_ref, sem)


def in_vmem(count):
    return [pl.BlockSpec(memory_space=pltpu.VMEM)] * count


def anywhere(count):
    return [pl.BlockSpec(memory_space=pl.ANY)] * count


def cost(flops, size):
    return pl.CostEstimate(flops=flops, bytes_accessed=size, transcendentals=0)


def room(mib):
    return pltpu.CompilerParams(vmem_limit_bytes=mib << 20)


def on_device(links):
    slices, _, _, planes, cells = links.shape
    times_ta, parts_gx = lax.axis_size("ta"), lax.axis_size("gx")
    depth = times_ta.bit_length() - 1
    blocks = cells // LANES
    half = blocks // 2
    if times_ta != 1 << depth or depth < 3 or blocks % 2:
        raise ValueError("unsupported sizes")
    f32 = jnp.float32
    shape = lambda *s: jax.ShapeDtypeStruct(s, f32)
    sites = planes * cells
    size = state_rows(planes, half)
    tiles = 12 * half * planes

    def across(x, step):
        return lax.ppermute(x, "ta", [(i, i ^ (1 << step)) for i in range(times_ta)])

    keep, send, rim, side = pl.pallas_call(
        functools.partial(block_kernel, half),
        out_shape=(shape(tiles, LANES), shape(tiles, LANES),
                   shape(12 * half + 12 * blocks * (slices - 1), LANES), shape(12 * half, LANES)),
        in_specs=in_vmem(1),
        out_specs=tuple(in_vmem(4)),
        cost_estimate=cost(200 * sites, 90 * sites),
        compiler_params=room(8),
        name="block_product",
    )(links[:, 3])

    seen = across(send, 0)
    rim = lax.ppermute(rim, "gx", [(i, (i - 1) % parts_gx) for i in range(parts_gx)])
    side = lax.ppermute(
        side, ("ta", "gx"),
        [(i * parts_gx + j, (i ^ 1) * parts_gx + (j - 1) % parts_gx)
         for i in range(times_ta) for j in range(parts_gx)],
    )
    block, lower = pl.pallas_call(
        functools.partial(pair_kernel, planes, half),
        out_shape=(shape(size, LANES), shape(size, LANES)),
        in_specs=in_vmem(4),
        out_specs=tuple(in_vmem(2)),
        cost_estimate=cost(100 * sites, 50 * sites),
        compiler_params=room(8),
        name="pair",
    )(keep, seen, rim, side)

    prefix = None
    for step in range(1, depth - 1):
        first, last = step == 1, step == depth - 2
        seen = across(block, step)
        operands = [block, seen] + ([] if first else [prefix]) + ([lower] if last else [])
        outs = [shape(size, LANES)] * 2 + ([shape(2 * size, LANES)] if last else [])
        block, prefix, *pair = pl.pallas_call(
            functools.partial(combine_kernel, planes, half, step, first, last),
            out_shape=tuple(outs),
            in_specs=in_vmem(len(operands)),
            out_specs=tuple(in_vmem(len(outs))),
            cost_estimate=cost(200 * sites, 100 * sites),
            compiler_params=room(8),
            name="combine",
        )(*operands)

    step = depth - 1
    seen = across(block, step)
    pair = across(pair[0], 0)
    seen_back = across(seen, 0)

    def scratch(count):
        return [pltpu.VMEM((count, slices, 18, planes, LANES), f32),
                pltpu.VMEM((count, slices, planes, LANES), f32),
                pltpu.SemaphoreType.DMA((count, 2))]

    wide = (shape(slices, 3, 18, planes, cells), shape(slices, 3, planes, cells))
    fields = (shape(half, 18 * (slices + 1), planes, LANES), shape(18 * (slices + 1) * half, LANES))
    spatial, correlator, field, edge = pl.pallas_call(
        functools.partial(early_kernel, planes, half, step),
        out_shape=wide + fields,
        in_specs=in_vmem(5),
        out_specs=tuple(anywhere(2) + in_vmem(2)),
        scratch_shapes=scratch(len(jobs_of(half, False))),
        cost_estimate=cost(2000 * sites, 400 * sites),
        compiler_params=room(12),
        name="early",
    )(links, block, prefix, seen, rim)
    return pl.pallas_call(
        functools.partial(late_kernel, planes, half, step),
        out_shape=wide,
        in_specs=in_vmem(6) + anywhere(2),
        out_specs=tuple(anywhere(2)),
        input_output_aliases={6: 0, 7: 1},
        scratch_shapes=[pltpu.VMEM(f.shape, f32) for f in fields] + scratch(len(jobs_of(half, True))),
        cost_estimate=cost(2500 * sites, 600 * sites),
        compiler_params=room(12),
        name="late",
    )(links, pair, seen_back, rim, field, edge, spatial, correlator)


def solution(mesh):
    in_specs = (P("ta", None, None, "gx", None),)
    out_specs = (P("ta", None, None, "gx", None), P("ta", None, "gx", None))
    return jax.shard_map(on_device, mesh=mesh, in_specs=in_specs, out_specs=out_specs, check_vma=False)
```

```python
import functools

import jax
import jax.numpy as jnp
from jax import lax
from jax.experimental import pallas as pl
from jax.experimental.pallas import tpu as pltpu
from jax.sharding import PartitionSpec as P

LZ = 32
LANES = 128


def total(terms):
    result = terms[0]
    for term in terms[1:]:
        result = result + term
    return result


def dot(left, right):
    pairs = list(zip(left, right))
    real = total([a[0] * b[0] for a, b in pairs]) - total([a[1] * b[1] for a, b in pairs])
    imag = total([a[0] * b[1] for a, b in pairs] + [a[1] * b[0] for a, b in pairs])
    return real, imag


def dot_conj(left, right):
    pairs = list(zip(left, right))
    real = total([a[0] * b[0] for a, b in pairs] + [a[1] * b[1] for a, b in pairs])
    imag = total([a[1] * b[0] for a, b in pairs]) - total([a[0] * b[1] for a, b in pairs])
    return real, imag


def times(rows, matrix):
    columns = [[matrix[k][j] for k in range(3)] for j in range(3)]
    return [[dot(row, column) for column in columns] for row in rows]


def times_dagger(rows, matrix):
    return [[dot_conj(row, other) for other in matrix] for row in rows]


def complete(rows):
    first, second = rows[0], rows[1]
    third = []
    for j in range(3):
        a, b = (j + 1) % 3, (j + 2) % 3
        ar, ai = first[a]
        br, bi = second[b]
        cr, ci = first[b]
        dr, di = second[a]
        third.append((ar * br - ai * bi - cr * dr + ci * di, cr * di + ci * dr - ar * bi - ai * br))
    return [first, second, third]


def pick(flag, yes, no):
    return [
        [(jnp.where(flag, y[0], n[0]), jnp.where(flag, y[1], n[1])) for y, n in zip(yr, nr)]
        for yr, nr in zip(yes, no)
    ]


def unit_rows(like):
    one, zero = jnp.ones_like(like), jnp.zeros_like(like)
    return [[(one if i == j else zero, zero) for j in range(3)] for i in range(2)]


def trace_of_product(left, right):
    reals = total([left[i][j][0] * right[j][i][0] for i in range(3) for j in range(3)])
    return reals - total([left[i][j][1] * right[j][i][1] for i in range(3) for j in range(3)])


def matrix_at(at, rows):
    return [[(at(i * 3 + j), at((rows + i) * 3 + j)) for j in range(3)] for i in range(rows)]


def put(at, matrix):
    rows = len(matrix)
    for i in range(rows):
        for j in range(3):
            at(i * 3 + j, matrix[i][j][0])
            at((rows + i) * 3 + j, matrix[i][j][1])


def groups(planes, half):
    return [lambda k, block=block: pl.ds((k * half + block) * planes, planes) for block in range(half)]


def edge_groups(planes, half):
    return [lambda k, block=block: pl.ds((k * half + block) * planes, 1) for block in range(half)]


def take(ref, rows, base=0):
    return matrix_at(lambda k: ref[pl.ds(rows(k).start + base, rows(k).size), :], 2)


def give(ref, rows, matrix, base=0):
    def at(k, value):
        ref[pl.ds(rows(k).start + base, rows(k).size), :] = value
    put(at, matrix)


def bit_of(step):
    return lax.rem(lax.axis_index("ta") // (1 << step), 2)


def lane_block(c):
    return pl.ds(pl.multiple_of(c * LANES, LANES), LANES)


def block_kernel(half, links_ref, keep_ref, send_ref, raw_ref):
    slices, _, planes, cells = links_ref.shape
    blocks = cells // LANES
    own = bit_of(0)
    for which in range(2):
        for block in range(half):
            c = (own if which == 0 else 1 - own) * half + block
            at = lane_block(c)
            link = lambda t: matrix_at(lambda k: links_ref[t, k, :, at], 3)
            rows = link(0)[:2]
            for t in range(1, slices):
                def edge(k, value):
                    raw_ref[pl.ds((12 * (t - 1) + k) * blocks + c, 1), :] = value
                put(edge, [[(v[0][:1], v[1][:1]) for v in row] for row in link(t - 1)[:2]])
                rows = times(rows, link(t))
            give(keep_ref if which == 0 else send_ref, groups(planes, half)[block], rows)


def pair_kernel(planes, half, keep_ref, seen_ref, block_ref, lower_ref):
    upper = bit_of(0) == 1
    for rows in groups(planes, half):
        own, seen = take(keep_ref, rows), take(seen_ref, rows)
        low, high = pick(upper, seen, own), pick(upper, own, seen)
        give(block_ref, rows, times(low, complete(high)))
        give(lower_ref, rows, low)


def combine_kernel(planes, half, step, first, last, *refs):
    refs = list(refs)
    block_ref, seen_ref = refs.pop(0), refs.pop(0)
    prefix_ref = None if first else refs.pop(0)
    lower_ref = refs.pop(0) if last else None
    flag = bit_of(step) == 1
    odd = bit_of(0) == 1
    for rows in groups(planes, half):
        own, seen = take(block_ref, rows), take(seen_ref, rows)
        block = times(pick(flag, seen, own), complete(pick(flag, own, seen)))
        if first:
            prefix = pick(flag, seen, unit_rows(seen[0][0][0]))
        else:
            before = take(prefix_ref, rows)
            prefix = pick(flag, times(seen, complete(before)), before)
        give(refs[0], rows, block)
        if last:
            after = times(prefix, complete(take(lower_ref, rows)))
            give(refs[1], rows, pick(odd, after, prefix))
            give(refs[2], rows, block)
            give(refs[2], rows, pick(odd, prefix, after), 12 * half * planes)
        else:
            give(refs[1], rows, prefix)


def close(flag, block, prefix, seen):
    poly = times(pick(flag, seen, block), complete(pick(flag, block, seen)))
    return poly, pick(flag, times(seen, complete(prefix)), prefix)


def edge_kernel(planes, half, step, block_ref, prefix_ref, pair_ref, seen_ref, raw_ref, here_ref, side_ref):
    flag = bit_of(step) == 1
    rows_of = 12 * half
    for index, rows in enumerate(edge_groups(planes, half)):
        poly, prefix = close(flag, take(block_ref, rows), take(prefix_ref, rows), take(seen_ref, rows))
        partner = take(pair_ref, rows, rows_of * planes)
        partner = pick(flag, times(take(seen_ref, rows), complete(partner)), partner)
        row = lambda k: pl.ds(k * half + index, 1)
        for ref, gauge in ((here_ref, prefix), (side_ref, partner)):
            give(ref, row, poly)
            give(ref, row, gauge, rows_of)
    here_ref[2 * rows_of:, :] = raw_ref[...]


def prepare(planes, half, step, other, links_ref, block, prefix, seen, field_ref):
    slices = links_ref.shape[0]
    flag = bit_of(step) == 1
    own = bit_of(0)
    for local, rows in enumerate(groups(planes, half)):
        at = lane_block((1 - own if other else own) * half + local)
        poly, gauge = close(flag, block(rows), prefix(rows), seen(rows))
        for t in range(slices + 1):
            if 0 < t < slices:
                gauge = times(gauge, matrix_at(lambda k: links_ref[t - 1, 3, k, :, at], 3))
            def store(k, v):
                field_ref[local, 18 * t + k] = v
            put(store, complete(gauge if t < slices else poly))


def prepare_edge(half, slices, blocks, other, edge_ref, raw_ref, out_ref):
    rows_of = 12 * half
    own = bit_of(0)
    start = (1 - own if other else own) * half
    rows = lambda k: pl.ds(k * half, half)
    poly, gauge = take(edge_ref, rows), take(edge_ref, rows, rows_of)
    for t in range(slices + 1):
        if 0 < t < slices:
            base = 2 * rows_of + 12 * blocks * (t - 1)
            link = matrix_at(lambda k: raw_ref[pl.ds(base + k * blocks + start, half), :], 2)
            gauge = times(gauge, complete(link))
        def store(k, v):
            out_ref[pl.ds((18 * t + k) * half, half), :] = v
        put(store, complete(gauge if t < slices else poly))


def shifted(load, direction, r, edge):
    value = load(r)
    lane = lax.broadcasted_iota(jnp.int32, value.shape, 1)
    if direction == 0:
        row = lax.broadcasted_iota(jnp.int32, value.shape, 0)
        mixed = jnp.where(row == 0, jnp.broadcast_to(edge(r), value.shape), value)
        return pltpu.roll(mixed, value.shape[0] - 1, 0)
    if direction == 1:
        mixed = jnp.where(lane < LZ, load(r + 1), value)
        return pltpu.roll(mixed, LANES - LZ, 1)
    ahead = pltpu.roll(value, LANES - 1, 1)
    around = pltpu.roll(value, LZ - 1, 1)
    return jnp.where(lax.rem(lane, LZ) == LZ - 1, around, ahead)


def outputs(half, jobs, links_ref, fields, edges, out_ref, trace_ref, done):
    slices, cells = links_ref.shape[0], links_ref.shape[-1]
    blocks = cells // LANES
    own = bit_of(0)

    def field(r, k):
        r = r % blocks
        return fields[r // half][r % half, k]

    def edge(r, k):
        at = k * half + r % half
        return edges[r // half][at:at + 1, :]

    for job, (r, direction) in enumerate(jobs):
        at = lane_block(lax.rem(own * half + r, blocks))

        def neighbour(base):
            def one(k):
                return shifted(lambda q: field(q, base + k), direction, r, lambda q: edge(q, base + k))
            return matrix_at(one, 3)

        poly = matrix_at(lambda k: field(r, 18 * slices + k), 3)
        poly_next = neighbour(18 * slices)
        for t in range(slices):
            link = matrix_at(lambda k: links_ref[t, direction, k, :, at], 3)
            gauge = matrix_at(lambda k: field(r, 18 * t + k), 3)[:2]
            moved = complete(times_dagger(times(gauge, link), neighbour(18 * t)))
            def store(k, v):
                out_ref[job, t, k] = v
            put(store, moved)
            around = complete(times_dagger(times_dagger(moved[:2], poly_next), moved))
            trace_ref[job, t] = trace_of_product(poly, around)
        done(job)


def copies(half, jobs, out_ref, trace_ref, spatial_ref, correlator_ref, sem, job):
    r, direction = jobs[job]
    at = lane_block(lax.rem(bit_of(0) * half + r, 2 * half))
    return (
        pltpu.make_async_copy(out_ref.at[job], spatial_ref.at[:, direction, :, :, at], sem.at[job, 0]),
        pltpu.make_async_copy(trace_ref.at[job], correlator_ref.at[:, direction, :, at], sem.at[job, 1]),
    )


def jobs_of(half, late):
    early = [(r, 2) for r in range(half)] + [(r, 1) for r in range(half - 1)]
    rest = [(r, d) for r in range(2 * half) for d in range(3) if (r, d) not in early]
    return rest if late else early


def early_kernel(planes, half, step, links_ref, block_ref, prefix_ref, seen_ref, field_ref, out_ref, trace_ref):
    prepare(planes, half, step, False, links_ref, lambda g: take(block_ref, g),
            lambda g: take(prefix_ref, g), lambda g: take(seen_ref, g), field_ref)
    outputs(half, jobs_of(half, False), links_ref, [field_ref, field_ref], None, out_ref, trace_ref, lambda job: None)


def late_kernel(planes, half, step, links_ref, pair_ref, seen_ref, here_ref, side_ref, field_ref, out_early,
                trace_early, spatial_ref, correlator_ref, field_late, edge_own, edge_late, out_ref, trace_ref,
                sem_early, sem):
    slices, blocks = links_ref.shape[0], links_ref.shape[-1] // LANES
    first = functools.partial(copies, half, jobs_of(half, False), out_early, trace_early,
                              spatial_ref, correlator_ref, sem_early)
    second = functools.partial(copies, half, jobs_of(half, True), out_ref, trace_ref,
                               spatial_ref, correlator_ref, sem)
    for job in range(len(jobs_of(half, False))):
        for copy in first(job):
            copy.start()
    size = 12 * half * planes
    prepare(planes, half, step, True, links_ref, lambda g: take(pair_ref, g),
            lambda g: take(pair_ref, g, size), lambda g: take(seen_ref, g), field_late)
    prepare_edge(half, slices, blocks, False, here_ref, here_ref, edge_own)
    prepare_edge(half, slices, blocks, True, side_ref, here_ref, edge_late)

    def done(job):
        for copy in second(job):
            copy.start()

    outputs(half, jobs_of(half, True), links_ref, [field_ref, field_late], [edge_own, edge_late],
            out_ref, trace_ref, done)
    for count, make in ((len(jobs_of(half, False)), first), (len(jobs_of(half, True)), second)):
        for job in range(count):
            for copy in make(job):
                copy.wait()


def in_vmem(count):
    return [pl.BlockSpec(memory_space=pltpu.VMEM)] * count


def anywhere(count):
    return [pl.BlockSpec(memory_space=pl.ANY)] * count


def cost(flops, size):
    return pl.CostEstimate(flops=flops, bytes_accessed=size, transcendentals=0)


def room(mib):
    return pltpu.CompilerParams(vmem_limit_bytes=mib << 20)


def on_device(links):
    slices, _, _, planes, cells = links.shape
    times_ta, parts_gx = lax.axis_size("ta"), lax.axis_size("gx")
    depth = times_ta.bit_length() - 1
    blocks = cells // LANES
    half = blocks // 2
    if times_ta != 1 << depth or depth < 3 or blocks % 2:
        raise ValueError("unsupported sizes")
    f32 = jnp.float32
    shape = lambda *s: jax.ShapeDtypeStruct(s, f32)
    sites = planes * cells
    size = 12 * half * planes
    raw_rows = 12 * blocks * (slices - 1)

    def across(x, step):
        return lax.ppermute(x, "ta", [(i, i ^ (1 << step)) for i in range(times_ta)])

    keep, send, raw = pl.pallas_call(
        functools.partial(block_kernel, half),
        out_shape=(shape(size, LANES), shape(size, LANES), shape(max(raw_rows, 8), LANES)),
        in_specs=in_vmem(1),
        out_specs=tuple(in_vmem(3)),
        cost_estimate=cost(200 * sites, 90 * sites),
        compiler_params=room(8),
        name="block_product",
    )(links[:, 3])

    seen = across(send, 0)
    block, lower = pl.pallas_call(
        functools.partial(pair_kernel, planes, half),
        out_shape=(shape(size, LANES), shape(size, LANES)),
        in_specs=in_vmem(2),
        out_specs=tuple(in_vmem(2)),
        cost_estimate=cost(100 * sites, 50 * sites),
        compiler_params=room(8),
        name="pair",
    )(keep, seen)

    prefix = None
    for step in range(1, depth - 1):
        first, last = step == 1, step == depth - 2
        seen = across(block, step)
        operands = [block, seen] + ([] if first else [prefix]) + ([lower] if last else [])
        outs = [shape(size, LANES)] * 2 + ([shape(2 * size, LANES)] if last else [])
        block, prefix, *pair = pl.pallas_call(
            functools.partial(combine_kernel, planes, half, step, first, last),
            out_shape=tuple(outs),
            in_specs=in_vmem(len(operands)),
            out_specs=tuple(in_vmem(len(outs))),
            cost_estimate=cost(200 * sites, 100 * sites),
            compiler_params=room(8),
            name="combine",
        )(*operands)

    step = depth - 1
    seen = across(block, step)
    pair = pair[0]
    pair_back = across(pair, 0)
    seen_back = across(seen, 0)

    here, side = pl.pallas_call(
        functools.partial(edge_kernel, planes, half, step),
        out_shape=(shape(24 * half + max(raw_rows, 8), LANES), shape(24 * half, LANES)),
        in_specs=in_vmem(5),
        out_specs=tuple(in_vmem(2)),
        cost_estimate=cost(20 * sites, 10 * sites),
        compiler_params=room(8),
        name="edge",
    )(block, prefix, pair, seen, raw)
    here = lax.ppermute(here, "gx", [(i, (i - 1) % parts_gx) for i in range(parts_gx)])
    side = lax.ppermute(
        side, ("ta", "gx"),
        [(i * parts_gx + j, (i ^ 1) * parts_gx + (j - 1) % parts_gx)
         for i in range(times_ta) for j in range(parts_gx)],
    )

    def results(count):
        return [(count, slices, 18, planes, LANES), (count, slices, planes, LANES)]

    early, late = len(jobs_of(half, False)), len(jobs_of(half, True))
    field_shape = (half, 18 * (slices + 1), planes, LANES)
    field, out, trace = pl.pallas_call(
        functools.partial(early_kernel, planes, half, step),
        out_shape=tuple(shape(*s) for s in [field_shape] + results(early)),
        in_specs=in_vmem(4),
        out_specs=tuple(in_vmem(3)),
        cost_estimate=cost(2000 * sites, 400 * sites),
        compiler_params=room(8),
        name="early",
    )(links, block, prefix, seen)
    edge_shape = (18 * (slices + 1) * half, LANES)
    return pl.pallas_call(
        functools.partial(late_kernel, planes, half, step),
        out_shape=(shape(slices, 3, 18, planes, cells), shape(slices, 3, planes, cells)),
        in_specs=in_vmem(8),
        out_specs=tuple(anywhere(2)),
        scratch_shapes=[pltpu.VMEM(s, f32) for s in [field_shape, edge_shape, edge_shape] + results(late)]
        + [pltpu.SemaphoreType.DMA((early, 2)), pltpu.SemaphoreType.DMA((late, 2))],
        cost_estimate=cost(2500 * sites, 600 * sites),
        compiler_params=room(12),
        name="late",
    )(links, pair_back, seen_back, here, side, field, out, trace)


def solution(mesh):
    in_specs = (P("ta", None, None, "gx", None),)
    out_specs = (P("ta", None, None, "gx", None), P("ta", None, "gx", None))
    return jax.shard_map(on_device, mesh=mesh, in_specs=in_specs, out_specs=out_specs, check_vma=False)
```

```python
import functools

import jax
import jax.numpy as jnp
from jax import lax
from jax.experimental import pallas as pl
from jax.experimental.pallas import tpu as pltpu
from jax.sharding import PartitionSpec as P

LZ = 32
LANES = 128


def total(terms):
    result = terms[0]
    for term in terms[1:]:
        result = result + term
    return result


def dot(left, right):
    pairs = list(zip(left, right))
    real = total([a[0] * b[0] for a, b in pairs]) - total([a[1] * b[1] for a, b in pairs])
    imag = total([a[0] * b[1] for a, b in pairs] + [a[1] * b[0] for a, b in pairs])
    return real, imag


def dot_conj(left, right):
    pairs = list(zip(left, right))
    real = total([a[0] * b[0] for a, b in pairs] + [a[1] * b[1] for a, b in pairs])
    imag = total([a[1] * b[0] for a, b in pairs]) - total([a[0] * b[1] for a, b in pairs])
    return real, imag


def times(rows, matrix):
    columns = [[matrix[k][j] for k in range(3)] for j in range(3)]
    return [[dot(row, column) for column in columns] for row in rows]


def times_dagger(rows, matrix):
    return [[dot_conj(row, other) for other in matrix] for row in rows]


def complete(rows):
    first, second = rows[0], rows[1]
    third = []
    for j in range(3):
        a, b = (j + 1) % 3, (j + 2) % 3
        ar, ai = first[a]
        br, bi = second[b]
        cr, ci = first[b]
        dr, di = second[a]
        third.append((ar * br - ai * bi - cr * dr + ci * di, cr * di + ci * dr - ar * bi - ai * br))
    return [first, second, third]


def pick(flag, yes, no):
    return [
        [(jnp.where(flag, y[0], n[0]), jnp.where(flag, y[1], n[1])) for y, n in zip(yr, nr)]
        for yr, nr in zip(yes, no)
    ]


def unit_rows(like):
    one, zero = jnp.ones_like(like), jnp.zeros_like(like)
    return [[(one if i == j else zero, zero) for j in range(3)] for i in range(2)]


def trace_of_product(left, right):
    reals = total([left[i][j][0] * right[j][i][0] for i in range(3) for j in range(3)])
    return reals - total([left[i][j][1] * right[j][i][1] for i in range(3) for j in range(3)])


def matrix_at(at, rows):
    return [[(at(i * 3 + j), at((rows + i) * 3 + j)) for j in range(3)] for i in range(rows)]


def put(at, matrix):
    rows = len(matrix)
    for i in range(rows):
        for j in range(3):
            at(i * 3 + j, matrix[i][j][0])
            at((rows + i) * 3 + j, matrix[i][j][1])


def groups(planes, half):
    return [lambda k, block=block: pl.ds((k * half + block) * planes, planes) for block in range(half)]


def edge_groups(planes, half):
    return [lambda k, block=block: pl.ds((k * half + block) * planes, 1) for block in range(half)]


def take(ref, rows, base=0):
    return matrix_at(lambda k: ref[pl.ds(rows(k).start + base, rows(k).size), :], 2)


def give(ref, rows, matrix, base=0):
    def at(k, value):
        ref[pl.ds(rows(k).start + base, rows(k).size), :] = value
    put(at, matrix)


def bit_of(step):
    return lax.rem(lax.axis_index("ta") // (1 << step), 2)


def lane_block(c):
    return pl.ds(pl.multiple_of(c * LANES, LANES), LANES)


def block_kernel(half, links_ref, keep_ref, send_ref, raw_ref):
    slices, _, planes, cells = links_ref.shape
    blocks = cells // LANES
    own = bit_of(0)
    for which in range(2):
        for block in range(half):
            c = (own if which == 0 else 1 - own) * half + block
            at = lane_block(c)
            link = lambda t: matrix_at(lambda k: links_ref[t, k, :, at], 3)
            rows = link(0)[:2]
            for t in range(1, slices):
                def edge(k, value):
                    raw_ref[pl.ds((12 * (t - 1) + k) * blocks + c, 1), :] = value
                put(edge, [[(v[0][:1], v[1][:1]) for v in row] for row in link(t - 1)[:2]])
                rows = times(rows, link(t))
            give(keep_ref if which == 0 else send_ref, groups(planes, half)[block], rows)


def pair_kernel(planes, half, keep_ref, seen_ref, block_ref, lower_ref):
    upper = bit_of(0) == 1
    for rows in groups(planes, half):
        own, seen = take(keep_ref, rows), take(seen_ref, rows)
        low, high = pick(upper, seen, own), pick(upper, own, seen)
        give(block_ref, rows, times(low, complete(high)))
        give(lower_ref, rows, low)


def combine_kernel(planes, half, step, first, last, *refs):
    refs = list(refs)
    block_ref, seen_ref = refs.pop(0), refs.pop(0)
    prefix_ref = None if first else refs.pop(0)
    lower_ref = refs.pop(0) if last else None
    flag = bit_of(step) == 1
    odd = bit_of(0) == 1
    for rows in groups(planes, half):
        own, seen = take(block_ref, rows), take(seen_ref, rows)
        block = times(pick(flag, seen, own), complete(pick(flag, own, seen)))
        if first:
            prefix = pick(flag, seen, unit_rows(seen[0][0][0]))
        else:
            before = take(prefix_ref, rows)
            prefix = pick(flag, times(seen, complete(before)), before)
        give(refs[0], rows, block)
        if last:
            after = times(prefix, complete(take(lower_ref, rows)))
            give(refs[1], rows, pick(odd, after, prefix))
            give(refs[2], rows, block)
            give(refs[2], rows, pick(odd, prefix, after), 12 * half * planes)
        else:
            give(refs[1], rows, prefix)


def close(flag, block, prefix, seen):
    poly = times(pick(flag, seen, block), complete(pick(flag, block, seen)))
    return poly, pick(flag, times(seen, complete(prefix)), prefix)


def edge_kernel(planes, half, step, block_ref, prefix_ref, pair_ref, seen_ref, raw_ref, here_ref, side_ref):
    flag = bit_of(step) == 1
    rows_of = 12 * half
    for index, rows in enumerate(edge_groups(planes, half)):
        poly, prefix = close(flag, take(block_ref, rows), take(prefix_ref, rows), take(seen_ref, rows))
        partner = take(pair_ref, rows, rows_of * planes)
        partner = pick(flag, times(take(seen_ref, rows), complete(partner)), partner)
        row = lambda k: pl.ds(k * half + index, 1)
        for ref, gauge in ((here_ref, prefix), (side_ref, partner)):
            give(ref, row, poly)
            give(ref, row, gauge, rows_of)
    here_ref[2 * rows_of:, :] = raw_ref[...]


def prepare(planes, half, step, other, links_ref, block, prefix, seen, field_ref):
    slices = links_ref.shape[0]
    flag = bit_of(step) == 1
    own = bit_of(0)
    for local, rows in enumerate(groups(planes, half)):
        at = lane_block((1 - own if other else own) * half + local)
        poly, gauge = close(flag, block(rows), prefix(rows), seen(rows))
        for t in range(slices + 1):
            if 0 < t < slices:
                gauge = times(gauge, matrix_at(lambda k: links_ref[t - 1, 3, k, :, at], 3))
            def store(k, v):
                field_ref[local, 18 * t + k] = v
            put(store, complete(gauge if t < slices else poly))


def prepare_edge(half, slices, blocks, other, edge_ref, raw_ref, out_ref):
    rows_of = 12 * half
    own = bit_of(0)
    start = (1 - own if other else own) * half
    rows = lambda k: pl.ds(k * half, half)
    poly, gauge = take(edge_ref, rows), take(edge_ref, rows, rows_of)
    for t in range(slices + 1):
        if 0 < t < slices:
            base = 2 * rows_of + 12 * blocks * (t - 1)
            link = matrix_at(lambda k: raw_ref[pl.ds(base + k * blocks + start, half), :], 2)
            gauge = times(gauge, complete(link))
        def store(k, v):
            out_ref[pl.ds((18 * t + k) * half, half), :] = v
        put(store, complete(gauge if t < slices else poly))


def shifted(load, direction, r, edge):
    value = load(r)
    lane = lax.broadcasted_iota(jnp.int32, value.shape, 1)
    if direction == 0:
        row = lax.broadcasted_iota(jnp.int32, value.shape, 0)
        mixed = jnp.where(row == 0, jnp.broadcast_to(edge(r), value.shape), value)
        return pltpu.roll(mixed, value.shape[0] - 1, 0)
    if direction == 1:
        mixed = jnp.where(lane < LZ, load(r + 1), value)
        return pltpu.roll(mixed, LANES - LZ, 1)
    ahead = pltpu.roll(value, LANES - 1, 1)
    around = pltpu.roll(value, LZ - 1, 1)
    return jnp.where(lax.rem(lane, LZ) == LZ - 1, around, ahead)


def outputs(half, jobs, links_ref, fields, edges, out_ref, trace_ref, done):
    slices, cells = links_ref.shape[0], links_ref.shape[-1]
    blocks = cells // LANES
    own = bit_of(0)

    def field(r, k):
        r = r % blocks
        return fields[r // half][r % half, k]

    def edge(r, k):
        at = k * half + r % half
        return edges[r // half][at:at + 1, :]

    for job, (r, direction) in enumerate(jobs):
        at = lane_block(lax.rem(own * half + r, blocks))

        def neighbour(base):
            def one(k):
                return shifted(lambda q: field(q, base + k), direction, r, lambda q: edge(q, base + k))
            return matrix_at(one, 3)

        poly = matrix_at(lambda k: field(r, 18 * slices + k), 3)
        poly_next = neighbour(18 * slices)
        for t in range(slices):
            link = matrix_at(lambda k: links_ref[t, direction, k, :, at], 3)
            gauge = matrix_at(lambda k: field(r, 18 * t + k), 3)[:2]
            moved = complete(times_dagger(times(gauge, link), neighbour(18 * t)))
            def store(k, v):
                out_ref[job, t, k] = v
            put(store, moved)
            around = complete(times_dagger(times_dagger(moved[:2], poly_next), moved))
            trace_ref[job, t] = trace_of_product(poly, around)
        done(job)


def copies(half, jobs, out_ref, trace_ref, spatial_ref, correlator_ref, sem, job):
    r, direction = jobs[job]
    at = lane_block(lax.rem(bit_of(0) * half + r, 2 * half))
    return (
        pltpu.make_async_copy(out_ref.at[job], spatial_ref.at[:, direction, :, :, at], sem.at[job, 0]),
        pltpu.make_async_copy(trace_ref.at[job], correlator_ref.at[:, direction, :, at], sem.at[job, 1]),
    )


def jobs_of(half, stage):
    early = [(r, 2) for r in range(half)] + [(r, 1) for r in range(half - 1)]
    late = [(half - 1, 1)] + [(r, d) for r in range(half, 2 * half) for d in (1, 2)]
    return (early, late, [(r, 0) for r in range(2 * half)])[stage]


def early_kernel(planes, half, step, links_ref, block_ref, prefix_ref, seen_ref, field_ref, out_ref, trace_ref):
    prepare(planes, half, step, False, links_ref, lambda g: take(block_ref, g),
            lambda g: take(prefix_ref, g), lambda g: take(seen_ref, g), field_ref)
    outputs(half, jobs_of(half, 0), links_ref, [field_ref, field_ref], None, out_ref, trace_ref, lambda job: None)


def late_kernel(planes, half, step, links_ref, pair_ref, seen_ref, field_own, field_ref, out_ref, trace_ref):
    size = 12 * half * planes
    prepare(planes, half, step, True, links_ref, lambda g: take(pair_ref, g),
            lambda g: take(pair_ref, g, size), lambda g: take(seen_ref, g), field_ref)
    outputs(half, jobs_of(half, 1), links_ref, [field_own, field_ref], None, out_ref, trace_ref, lambda job: None)


def last_kernel(half, links_ref, here_ref, side_ref, field_own, field_other, out_early, trace_early,
                out_late, trace_late, spatial_ref, correlator_ref, edge_own, edge_other, out_ref, trace_ref,
                sem_early, sem_late, sem):
    slices, blocks = links_ref.shape[0], links_ref.shape[-1] // LANES
    made = []
    for stage, refs in enumerate(((out_early, trace_early, sem_early), (out_late, trace_late, sem_late),
                                  (out_ref, trace_ref, sem))):
        out, trace, flags = refs
        jobs = jobs_of(half, stage)
        made.append([copies(half, jobs, out, trace, spatial_ref, correlator_ref, flags, j) for j in range(len(jobs))])
    for pairs in made[:2]:
        for pair in pairs:
            for copy in pair:
                copy.start()
    prepare_edge(half, slices, blocks, False, here_ref, here_ref, edge_own)
    prepare_edge(half, slices, blocks, True, side_ref, here_ref, edge_other)

    def done(job):
        for copy in made[2][job]:
            copy.start()

    outputs(half, jobs_of(half, 2), links_ref, [field_own, field_other], [edge_own, edge_other],
            out_ref, trace_ref, done)
    for pairs in made:
        for pair in pairs:
            for copy in pair:
                copy.wait()


def in_vmem(count):
    return [pl.BlockSpec(memory_space=pltpu.VMEM)] * count


def anywhere(count):
    return [pl.BlockSpec(memory_space=pl.ANY)] * count


def cost(flops, size):
    return pl.CostEstimate(flops=flops, bytes_accessed=size, transcendentals=0)


def room(mib):
    return pltpu.CompilerParams(vmem_limit_bytes=mib << 20)


def on_device(links):
    slices, _, _, planes, cells = links.shape
    times_ta, parts_gx = lax.axis_size("ta"), lax.axis_size("gx")
    depth = times_ta.bit_length() - 1
    blocks = cells // LANES
    half = blocks // 2
    if times_ta != 1 << depth or depth < 3 or blocks % 2:
        raise ValueError("unsupported sizes")
    f32 = jnp.float32
    shape = lambda *s: jax.ShapeDtypeStruct(s, f32)
    sites = planes * cells
    size = 12 * half * planes
    raw_rows = 12 * blocks * (slices - 1)

    def across(x, step):
        return lax.ppermute(x, "ta", [(i, i ^ (1 << step)) for i in range(times_ta)])

    keep, send, raw = pl.pallas_call(
        functools.partial(block_kernel, half),
        out_shape=(shape(size, LANES), shape(size, LANES), shape(max(raw_rows, 8), LANES)),
        in_specs=in_vmem(1),
        out_specs=tuple(in_vmem(3)),
        cost_estimate=cost(200 * sites, 90 * sites),
        compiler_params=room(8),
        name="block_product",
    )(links[:, 3])

    seen = across(send, 0)
    block, lower = pl.pallas_call(
        functools.partial(pair_kernel, planes, half),
        out_shape=(shape(size, LANES), shape(size, LANES)),
        in_specs=in_vmem(2),
        out_specs=tuple(in_vmem(2)),
        cost_estimate=cost(100 * sites, 50 * sites),
        compiler_params=room(8),
        name="pair",
    )(keep, seen)

    prefix = None
    for step in range(1, depth - 1):
        first, last = step == 1, step == depth - 2
        seen = across(block, step)
        operands = [block, seen] + ([] if first else [prefix]) + ([lower] if last else [])
        outs = [shape(size, LANES)] * 2 + ([shape(2 * size, LANES)] if last else [])
        block, prefix, *pair = pl.pallas_call(
            functools.partial(combine_kernel, planes, half, step, first, last),
            out_shape=tuple(outs),
            in_specs=in_vmem(len(operands)),
            out_specs=tuple(in_vmem(len(outs))),
            cost_estimate=cost(200 * sites, 100 * sites),
            compiler_params=room(8),
            name="combine",
        )(*operands)

    step = depth - 1
    seen = across(block, step)
    pair = pair[0]
    pair_back = across(pair, 0)
    seen_back = across(seen, 0)

    here, side = pl.pallas_call(
        functools.partial(edge_kernel, planes, half, step),
        out_shape=(shape(24 * half + max(raw_rows, 8), LANES), shape(24 * half, LANES)),
        in_specs=in_vmem(5),
        out_specs=tuple(in_vmem(2)),
        cost_estimate=cost(20 * sites, 10 * sites),
        compiler_params=room(8),
        name="edge",
    )(block, prefix, pair, seen, raw)
    here = lax.ppermute(here, "gx", [(i, (i - 1) % parts_gx) for i in range(parts_gx)])
    side = lax.ppermute(
        side, ("ta", "gx"),
        [(i * parts_gx + j, (i ^ 1) * parts_gx + (j - 1) % parts_gx)
         for i in range(times_ta) for j in range(parts_gx)],
    )

    def results(count):
        return [(count, slices, 18, planes, LANES), (count, slices, planes, LANES)]

    counts = [len(jobs_of(half, stage)) for stage in range(3)]
    field_shape = (half, 18 * (slices + 1), planes, LANES)
    field_own, out_early, trace_early = pl.pallas_call(
        functools.partial(early_kernel, planes, half, step),
        out_shape=tuple(shape(*s) for s in [field_shape] + results(counts[0])),
        in_specs=in_vmem(4),
        out_specs=tuple(in_vmem(3)),
        cost_estimate=cost(1200 * sites, 400 * sites),
        compiler_params=room(8),
        name="early",
    )(links, block, prefix, seen)
    field_other, out_late, trace_late = pl.pallas_call(
        functools.partial(late_kernel, planes, half, step),
        out_shape=tuple(shape(*s) for s in [field_shape] + results(counts[1])),
        in_specs=in_vmem(4),
        out_specs=tuple(in_vmem(3)),
        cost_estimate=cost(2000 * sites, 600 * sites),
        compiler_params=room(8),
        name="late",
    )(links, pair_back, seen_back, field_own)
    edge_shape = (18 * (slices + 1) * half, LANES)
    return pl.pallas_call(
        functools.partial(last_kernel, half),
        out_shape=(shape(slices, 3, 18, planes, cells), shape(slices, 3, planes, cells)),
        in_specs=in_vmem(9),
        out_specs=tuple(anywhere(2)),
        scratch_shapes=[pltpu.VMEM(s, f32) for s in [edge_shape, edge_shape] + results(counts[2])]
        + [pltpu.SemaphoreType.DMA((count, 2)) for count in counts],
        cost_estimate=cost(1500 * sites, 600 * sites),
        compiler_params=room(12),
        name="last",
    )(links, here, side, field_own, field_other, out_early, trace_early, out_late, trace_late)


def solution(mesh):
    in_specs = (P("ta", None, None, "gx", None),)
    out_specs = (P("ta", None, None, "gx", None), P("ta", None, "gx", None))
    return jax.shard_map(on_device, mesh=mesh, in_specs=in_specs, out_specs=out_specs, check_vma=False)
```

```python
import functools

import jax
import jax.numpy as jnp
from jax import lax
from jax.experimental import pallas as pl
from jax.experimental.pallas import tpu as pltpu
from jax.sharding import PartitionSpec as P


LZ = 32
LANES = 128


def total(terms):
    result = terms[0]
    for term in terms[1:]:
        result = result + term
    return result


def dot(left, right):
    pairs = list(zip(left, right))
    real = total([a[0] * b[0] for a, b in pairs]) - total([a[1] * b[1] for a, b in pairs])
    imag = total([a[0] * b[1] for a, b in pairs] + [a[1] * b[0] for a, b in pairs])
    return real, imag


def dot_conj(left, right):
    pairs = list(zip(left, right))
    real = total([a[0] * b[0] for a, b in pairs] + [a[1] * b[1] for a, b in pairs])
    imag = total([a[1] * b[0] for a, b in pairs]) - total([a[0] * b[1] for a, b in pairs])
    return real, imag


def times(rows, matrix):
    columns = [[matrix[k][j] for k in range(3)] for j in range(3)]
    return [[dot(row, column) for column in columns] for row in rows]


def times_dagger(rows, matrix):
    return [[dot_conj(row, other) for other in matrix] for row in rows]


def complete(rows):
    first, second = rows[0], rows[1]
    third = []
    for j in range(3):
        a, b = (j + 1) % 3, (j + 2) % 3
        ar, ai = first[a]
        br, bi = second[b]
        cr, ci = first[b]
        dr, di = second[a]
        third.append((ar * br - ai * bi - cr * dr + ci * di, cr * di + ci * dr - ar * bi - ai * br))
    return [first, second, third]


def pick(flag, yes, no):
    return [
        [(jnp.where(flag, y[0], n[0]), jnp.where(flag, y[1], n[1])) for y, n in zip(yr, nr)]
        for yr, nr in zip(yes, no)
    ]


def unit_rows(like):
    one, zero = jnp.ones_like(like), jnp.zeros_like(like)
    return [[(one if i == j else zero, zero) for j in range(3)] for i in range(2)]


def trace_of_product(left, right):
    reals = total([left[i][j][0] * right[j][i][0] for i in range(3) for j in range(3)])
    return reals - total([left[i][j][1] * right[j][i][1] for i in range(3) for j in range(3)])


def matrix_at(at, rows):
    return [[(at(i * 3 + j), at((rows + i) * 3 + j)) for j in range(3)] for i in range(rows)]


def put(at, matrix):
    rows = len(matrix)
    for i in range(rows):
        for j in range(3):
            at(i * 3 + j, matrix[i][j][0])
            at((rows + i) * 3 + j, matrix[i][j][1])


def groups(planes, half):
    return [lambda k, block=block: pl.ds((k * half + block) * planes, planes) for block in range(half)]


def edge_groups(planes, half):
    return [lambda k, block=block: pl.ds((k * half + block) * planes, 1) for block in range(half)]


def take(ref, rows, base=0):
    return matrix_at(lambda k: ref[pl.ds(rows(k).start + base, rows(k).size), :], 2)


def give(ref, rows, matrix, base=0):
    def at(k, value):
        ref[pl.ds(rows(k).start + base, rows(k).size), :] = value

    put(at, matrix)


def bit_of(step):
    return lax.rem(lax.axis_index("ta") // (1 << step), 2)


def lane_block(c):
    return pl.ds(pl.multiple_of(c * LANES, LANES), LANES)


def block_kernel(half, whole_ref, keep_ref, send_ref, raw_ref, links_ref, sem):
    copy = pltpu.make_async_copy(whole_ref.at[:, 3], links_ref, sem)
    copy.start()
    copy.wait()
    slices, _, planes, cells = links_ref.shape
    blocks = cells // LANES
    own = bit_of(0)
    for which in range(2):
        for block in range(half):
            c = (own if which == 0 else 1 - own) * half + block
            at = lane_block(c)
            link = lambda t: matrix_at(lambda k: links_ref[t, k, :, at], 3)
            rows = link(0)[:2]
            for t in range(1, slices):
                def edge(k, value):
                    raw_ref[pl.ds((12 * (t - 1) + k) * blocks + c, 1), :] = value

                put(edge, [[(v[0][:1], v[1][:1]) for v in row] for row in link(t - 1)[:2]])
                rows = times(rows, link(t))
            give(keep_ref if which == 0 else send_ref, groups(planes, half)[block], rows)


def pair_kernel(planes, half, keep_ref, seen_ref, block_ref, lower_ref):
    upper = bit_of(0) == 1
    for rows in groups(planes, half):
        own, seen = take(keep_ref, rows), take(seen_ref, rows)
        low, high = pick(upper, seen, own), pick(upper, own, seen)
        give(block_ref, rows, times(low, complete(high)))
        give(lower_ref, rows, low)


def combine_kernel(planes, half, step, first, last, *refs):
    refs = list(refs)
    block_ref, seen_ref = refs.pop(0), refs.pop(0)
    prefix_ref = None if first else refs.pop(0)
    lower_ref = refs.pop(0) if last else None
    flag = bit_of(step) == 1
    odd = bit_of(0) == 1
    for rows in groups(planes, half):
        own, seen = take(block_ref, rows), take(seen_ref, rows)
        block = times(pick(flag, seen, own), complete(pick(flag, own, seen)))
        if first:
            prefix = pick(flag, seen, unit_rows(seen[0][0][0]))
        else:
            before = take(prefix_ref, rows)
            prefix = pick(flag, times(seen, complete(before)), before)
        give(refs[0], rows, block)
        if last:
            after = times(prefix, complete(take(lower_ref, rows)))
            give(refs[1], rows, pick(odd, after, prefix))
            give(refs[2], rows, block)
            give(refs[2], rows, pick(odd, prefix, after), 12 * half * planes)
        else:
            give(refs[1], rows, prefix)


def close(flag, block, prefix, seen):
    poly = times(pick(flag, seen, block), complete(pick(flag, block, seen)))
    return poly, pick(flag, times(seen, complete(prefix)), prefix)


def edge_kernel(planes, half, step, block_ref, prefix_ref, pair_ref, seen_ref, raw_ref, here_ref, side_ref):
    flag = bit_of(step) == 1
    rows_of = 12 * half
    for index, rows in enumerate(edge_groups(planes, half)):
        poly, prefix = close(flag, take(block_ref, rows), take(prefix_ref, rows), take(seen_ref, rows))
        partner = take(pair_ref, rows, rows_of * planes)
        partner = pick(flag, times(take(seen_ref, rows), complete(partner)), partner)
        row = lambda k: pl.ds(k * half + index, 1)
        for ref, gauge in ((here_ref, prefix), (side_ref, partner)):
            give(ref, row, poly)
            give(ref, row, gauge, rows_of)
    here_ref[2 * rows_of:, :] = raw_ref[...]


def prepare(planes, half, step, other, links_ref, block, prefix, seen, field_ref):
    slices = links_ref.shape[0]
    flag = bit_of(step) == 1
    own = bit_of(0)
    for local, rows in enumerate(groups(planes, half)):
        at = lane_block((1 - own if other else own) * half + local)
        poly, gauge = close(flag, block(rows), prefix(rows), seen(rows))
        for t in range(slices + 1):
            if 0 < t < slices:
                gauge = times(gauge, matrix_at(lambda k: links_ref[t - 1, 3, k, :, at], 3))

            def store(k, v):
                field_ref[local, 18 * t + k] = v

            put(store, complete(gauge if t < slices else poly))


def prepare_edge(half, slices, blocks, other, edge_ref, raw_ref, out_ref):
    rows_of = 12 * half
    own = bit_of(0)
    start = (1 - own if other else own) * half
    rows = lambda k: pl.ds(k * half, half)
    poly, gauge = take(edge_ref, rows), take(edge_ref, rows, rows_of)
    for t in range(slices + 1):
        if 0 < t < slices:
            base = 2 * rows_of + 12 * blocks * (t - 1)
            link = matrix_at(lambda k: raw_ref[pl.ds(base + k * blocks + start, half), :], 2)
            gauge = times(gauge, complete(link))

        def store(k, v):
            out_ref[pl.ds((18 * t + k) * half, half), :] = v

        put(store, complete(gauge if t < slices else poly))


def shifted(load, direction, r, edge):
    value = load(r)
    lane = lax.broadcasted_iota(jnp.int32, value.shape, 1)
    if direction == 0:
        row = lax.broadcasted_iota(jnp.int32, value.shape, 0)
        mixed = jnp.where(row == 0, jnp.broadcast_to(edge(r), value.shape), value)
        return pltpu.roll(mixed, value.shape[0] - 1, 0)
    if direction == 1:
        mixed = jnp.where(lane < LZ, load(r + 1), value)
        return pltpu.roll(mixed, LANES - LZ, 1)
    ahead = pltpu.roll(value, LANES - 1, 1)
    around = pltpu.roll(value, LZ - 1, 1)
    return jnp.where(lax.rem(lane, LZ) == LZ - 1, around, ahead)


def outputs(half, jobs, links_ref, fields, edges, out_ref, trace_ref, done):
    slices, cells = links_ref.shape[0], links_ref.shape[-1]
    blocks = cells // LANES
    own = bit_of(0)

    def field(r, k):
        r = r % blocks
        return fields[r // half][r % half, k]

    def edge(r, k):
        at = k * half + r % half
        return edges[r // half][at:at + 1, :]

    for job, (r, direction) in enumerate(jobs):
        at = lane_block(lax.rem(own * half + r, blocks))

        def neighbour(base):
            def one(k):
                return shifted(lambda q: field(q, base + k), direction, r, lambda q: edge(q, base + k))

            return matrix_at(one, 3)

        poly = matrix_at(lambda k: field(r, 18 * slices + k), 3)
        poly_next = neighbour(18 * slices)
        for t in range(slices):
            link = matrix_at(lambda k: links_ref[t, direction, k, :, at], 3)
            gauge = matrix_at(lambda k: field(r, 18 * t + k), 3)[:2]
            moved = complete(times_dagger(times(gauge, link), neighbour(18 * t)))

            def store(k, v):
                out_ref[job, t, k] = v

            put(store, moved)
            around = complete(times_dagger(times_dagger(moved[:2], poly_next), moved))
            trace_ref[job, t] = trace_of_product(poly, around)
        done(job)


def copies(half, jobs, out_ref, trace_ref, spatial_ref, correlator_ref, sem, job):
    r, direction = jobs[job]
    at = lane_block(lax.rem(bit_of(0) * half + r, 2 * half))
    return (
        pltpu.make_async_copy(out_ref.at[job], spatial_ref.at[:, direction, :, :, at], sem.at[job, 0]),
        pltpu.make_async_copy(trace_ref.at[job], correlator_ref.at[:, direction, :, at], sem.at[job, 1]),
    )


def jobs_of(half, stage):
    early = [(r, 2) for r in range(half)] + [(r, 1) for r in range(half - 1)]
    late = [(half - 1, 1)] + [(r, d) for r in range(half, 2 * half) for d in (1, 2)]
    return (early, late, [(r, 0) for r in range(2 * half)])[stage]


def early_kernel(planes, half, step, links_ref, block_ref, prefix_ref, seen_ref, field_ref, out_ref, trace_ref):
    prepare(planes, half, step, False, links_ref, lambda g: take(block_ref, g),
            lambda g: take(prefix_ref, g), lambda g: take(seen_ref, g), field_ref)
    outputs(half, jobs_of(half, 0), links_ref, [field_ref, field_ref], None, out_ref, trace_ref, lambda job: None)


def late_kernel(planes, half, step, links_ref, pair_ref, seen_ref, field_own, field_ref, out_ref, trace_ref):
    size = 12 * half * planes
    prepare(planes, half, step, True, links_ref, lambda g: take(pair_ref, g),
            lambda g: take(pair_ref, g, size), lambda g: take(seen_ref, g), field_ref)
    outputs(half, jobs_of(half, 1), links_ref, [field_own, field_ref], None, out_ref, trace_ref, lambda job: None)


def last_kernel(half, links_ref, here_ref, side_ref, field_own, field_other, out_early, trace_early,
                out_late, trace_late, spatial_ref, correlator_ref, edge_own, edge_other, out_ref, trace_ref,
                sem_early, sem_late, sem):
    slices, blocks = links_ref.shape[0], links_ref.shape[-1] // LANES
    made = []
    for stage, refs in enumerate(((out_early, trace_early, sem_early), (out_late, trace_late, sem_late),
                                  (out_ref, trace_ref, sem))):
        out, trace, flags = refs
        jobs = jobs_of(half, stage)
        made.append([copies(half, jobs, out, trace, spatial_ref, correlator_ref, flags, j) for j in range(len(jobs))])
    for pairs in made[:2]:
        for pair in pairs:
            for copy in pair:
                copy.start()
    prepare_edge(half, slices, blocks, False, here_ref, here_ref, edge_own)
    prepare_edge(half, slices, blocks, True, side_ref, here_ref, edge_other)

    def done(job):
        for copy in made[2][job]:
            copy.start()

    outputs(half, jobs_of(half, 2), links_ref, [field_own, field_other], [edge_own, edge_other],
            out_ref, trace_ref, done)
    for pairs in made:
        for pair in pairs:
            for copy in pair:
                copy.wait()


def in_vmem(count):
    return [pl.BlockSpec(memory_space=pltpu.VMEM)] * count


def anywhere(count):
    return [pl.BlockSpec(memory_space=pl.ANY)] * count


def cost(flops, size):
    return pl.CostEstimate(flops=flops, bytes_accessed=size, transcendentals=0)


def room(mib):
    return pltpu.CompilerParams(vmem_limit_bytes=mib << 20)


def on_device(links):
    slices, _, _, planes, cells = links.shape
    times_ta, parts_gx = lax.axis_size("ta"), lax.axis_size("gx")
    depth = times_ta.bit_length() - 1
    blocks = cells // LANES
    half = blocks // 2
    if times_ta != 1 << depth or depth < 3 or blocks % 2:
        raise ValueError("unsupported sizes")
    f32 = jnp.float32
    shape = lambda *s: jax.ShapeDtypeStruct(s, f32)
    sites = planes * cells
    size = 12 * half * planes
    raw_rows = 12 * blocks * (slices - 1)

    def across(x, step):
        return lax.ppermute(x, "ta", [(i, i ^ (1 << step)) for i in range(times_ta)])

    keep, send, raw = pl.pallas_call(
        functools.partial(block_kernel, half),
        out_shape=(shape(size, LANES), shape(size, LANES), shape(max(raw_rows, 8), LANES)),
        in_specs=anywhere(1),
        out_specs=tuple(in_vmem(3)),
        scratch_shapes=[pltpu.VMEM((slices, 18, planes, cells), f32), pltpu.SemaphoreType.DMA],
        cost_estimate=cost(200 * sites, 90 * sites),
        compiler_params=room(8),
        name="block_product",
    )(pltpu.with_memory_space_constraint(links, pltpu.HBM))

    seen = across(send, 0)
    block, lower = pl.pallas_call(
        functools.partial(pair_kernel, planes, half),
        out_shape=(shape(size, LANES), shape(size, LANES)),
        in_specs=in_vmem(2),
        out_specs=tuple(in_vmem(2)),
        cost_estimate=cost(100 * sites, 50 * sites),
        compiler_params=room(8),
        name="pair",
    )(keep, seen)

    prefix = None
    for step in range(1, depth - 1):
        first, last = step == 1, step == depth - 2
        seen = across(block, step)
        operands = [block, seen] + ([] if first else [prefix]) + ([lower] if last else [])
        outs = [shape(size, LANES)] * 2 + ([shape(2 * size, LANES)] if last else [])
        block, prefix, *pair = pl.pallas_call(
            functools.partial(combine_kernel, planes, half, step, first, last),
            out_shape=tuple(outs),
            in_specs=in_vmem(len(operands)),
            out_specs=tuple(in_vmem(len(outs))),
            cost_estimate=cost(200 * sites, 100 * sites),
            compiler_params=room(8),
            name="combine",
        )(*operands)

    step = depth - 1
    seen = across(block, step)
    pair = pair[0]
    pair_back = across(pair, 0)
    seen_back = across(seen, 0)

    here, side = pl.pallas_call(
        functools.partial(edge_kernel, planes, half, step),
        out_shape=(shape(24 * half + max(raw_rows, 8), LANES), shape(24 * half, LANES)),
        in_specs=in_vmem(5),
        out_specs=tuple(in_vmem(2)),
        cost_estimate=cost(20 * sites, 10 * sites),
        compiler_params=room(8),
        name="edge",
    )(block, prefix, pair, seen, raw)
    here = lax.ppermute(here, "gx", [(i, (i - 1) % parts_gx) for i in range(parts_gx)])
    side = lax.ppermute(
        side, ("ta", "gx"),
        [(i * parts_gx + j, (i ^ 1) * parts_gx + (j - 1) % parts_gx)
         for i in range(times_ta) for j in range(parts_gx)],
    )

    def results(count):
        return [(count, slices, 18, planes, LANES), (count, slices, planes, LANES)]

    counts = [len(jobs_of(half, stage)) for stage in range(3)]
    field_shape = (half, 18 * (slices + 1), planes, LANES)
    field_own, out_early, trace_early = pl.pallas_call(
        functools.partial(early_kernel, planes, half, step),
        out_shape=tuple(shape(*s) for s in [field_shape] + results(counts[0])),
        in_specs=in_vmem(4),
        out_specs=tuple(in_vmem(3)),
        cost_estimate=cost(1200 * sites, 400 * sites),
        compiler_params=room(8),
        name="early",
    )(links, block, prefix, seen)
    field_other, out_late, trace_late = pl.pallas_call(
        functools.partial(late_kernel, planes, half, step),
        out_shape=tuple(shape(*s) for s in [field_shape] + results(counts[1])),
        in_specs=in_vmem(4),
        out_specs=tuple(in_vmem(3)),
        cost_estimate=cost(2000 * sites, 600 * sites),
        compiler_params=room(8),
        name="late",
    )(links, pair_back, seen_back, field_own)
    edge_shape = (18 * (slices + 1) * half, LANES)
    return pl.pallas_call(
        functools.partial(last_kernel, half),
        out_shape=(shape(slices, 3, 18, planes, cells), shape(slices, 3, planes, cells)),
        in_specs=in_vmem(9),
        out_specs=tuple(anywhere(2)),
        scratch_shapes=[pltpu.VMEM(s, f32) for s in [edge_shape, edge_shape] + results(counts[2])]
        + [pltpu.SemaphoreType.DMA((count, 2)) for count in counts],
        cost_estimate=cost(1500 * sites, 600 * sites),
        compiler_params=room(12),
        name="last",
    )(links, here, side, field_own, field_other, out_early, trace_early, out_late, trace_late)


def solution(mesh):
    in_specs = (P("ta", None, None, "gx", None),)
    out_specs = (P("ta", None, None, "gx", None), P("ta", None, "gx", None))
    return jax.shard_map(on_device, mesh=mesh, in_specs=in_specs, out_specs=out_specs, check_vma=False)
```

```python
import functools

import jax
import jax.numpy as jnp
from jax import lax
from jax.experimental import pallas as pl
from jax.experimental.pallas import tpu as pltpu
from jax.sharding import PartitionSpec as P


LZ = 32
LANES = 128


def total(terms):
    result = terms[0]
    for term in terms[1:]:
        result = result + term
    return result


def real_dot(left, right):
    return total([a * b for a, b in zip(left, right)])


def triples(rows, sign):
    return [([v[0] for v in row], [v[1] for v in row],
             [v[0] + v[1] if sign > 0 else v[0] - v[1] for v in row]) for row in rows]


def times(rows, matrix):
    columns = triples([[matrix[k][j] for k in range(3)] for j in range(3)], 1)
    result = []
    for left in triples(rows, 1):
        line = []
        for right in columns:
            a, b, c = (real_dot(x, y) for x, y in zip(left, right))
            line.append((a - b, c - a - b))
        result.append(line)
    return result


def times_dagger(rows, matrix):
    others = triples(matrix, -1)
    result = []
    for left in triples(rows, 1):
        line = []
        for right in others:
            a, b, c = (real_dot(x, y) for x, y in zip(left, right))
            line.append((a + b, c - a + b))
        result.append(line)
    return result


def complete(rows):
    first, second = rows[0], rows[1]
    third = []
    for j in range(3):
        a, b = (j + 1) % 3, (j + 2) % 3
        ar, ai = first[a]
        br, bi = second[b]
        cr, ci = first[b]
        dr, di = second[a]
        third.append((ar * br - ai * bi - cr * dr + ci * di, cr * di + ci * dr - ar * bi - ai * br))
    return [first, second, third]


def pick(flag, yes, no):
    return [
        [(jnp.where(flag, y[0], n[0]), jnp.where(flag, y[1], n[1])) for y, n in zip(yr, nr)]
        for yr, nr in zip(yes, no)
    ]


def unit_rows(like):
    one, zero = jnp.ones_like(like), jnp.zeros_like(like)
    return [[(one if i == j else zero, zero) for j in range(3)] for i in range(2)]


def trace_of_product(left, right):
    reals = total([left[i][j][0] * right[j][i][0] for i in range(3) for j in range(3)])
    return reals - total([left[i][j][1] * right[j][i][1] for i in range(3) for j in range(3)])


def matrix_at(at, rows):
    return [[(at(i * 3 + j), at((rows + i) * 3 + j)) for j in range(3)] for i in range(rows)]


def put(at, matrix):
    rows = len(matrix)
    for i in range(rows):
        for j in range(3):
            at(i * 3 + j, matrix[i][j][0])
            at((rows + i) * 3 + j, matrix[i][j][1])


def groups(planes, half):
    return [lambda k, block=block: pl.ds((k * half + block) * planes, planes) for block in range(half)]


def edge_groups(planes, half):
    return [lambda k, block=block: pl.ds((k * half + block) * planes, 1) for block in range(half)]


def take(ref, rows, base=0):
    return matrix_at(lambda k: ref[pl.ds(rows(k).start + base, rows(k).size), :], 2)


def give(ref, rows, matrix, base=0):
    def at(k, value):
        ref[pl.ds(rows(k).start + base, rows(k).size), :] = value

    put(at, matrix)


def bit_of(step):
    return lax.rem(lax.axis_index("ta") // (1 << step), 2)


def lane_block(c):
    return pl.ds(pl.multiple_of(c * LANES, LANES), LANES)


def block_kernel(half, which, whole_ref, block_ref, *rest):
    links_ref, sem = rest[-2:]
    slices, _, planes, cells = links_ref.shape
    blocks = whole_ref.shape[-1] // LANES
    own = bit_of(0)
    start = (own if which == 0 else 1 - own) * half if which else 0
    at = pl.ds(pl.multiple_of(start * LANES, LANES), cells)
    copy = pltpu.make_async_copy(whole_ref.at[:, 3, :, :, at], links_ref, sem)
    copy.start()
    copy.wait()
    for block in range(half):
        at = lane_block(block if which else own * half + block)
        link = lambda t: matrix_at(lambda k: links_ref[t, k, :, at], 3)
        rows = link(0)[:2]
        for t in range(1, slices):
            rows = times(rows, link(t))
        give(block_ref, groups(planes, half)[block], rows)
    if which == 0:
        for t in range(slices - 1):
            for c in range(blocks):
                def edge(k, value):
                    row = (12 * t + k) * blocks + c
                    rest[0][row:row + 1, :] = value[:1]

                put(edge, matrix_at(lambda k: links_ref[t, k, :, c * LANES:(c + 1) * LANES], 3)[:2])


def pair_kernel(planes, half, keep_ref, seen_ref, block_ref, lower_ref):
    upper = bit_of(0) == 1
    for rows in groups(planes, half):
        own, seen = take(keep_ref, rows), take(seen_ref, rows)
        low, high = pick(upper, seen, own), pick(upper, own, seen)
        give(block_ref, rows, times(low, complete(high)))
        give(lower_ref, rows, low)


def combine_kernel(planes, half, step, first, last, *refs):
    refs = list(refs)
    block_ref, seen_ref = refs.pop(0), refs.pop(0)
    prefix_ref = None if first else refs.pop(0)
    lower_ref = refs.pop(0) if last else None
    flag = bit_of(step) == 1
    odd = bit_of(0) == 1
    for rows in groups(planes, half):
        own, seen = take(block_ref, rows), take(seen_ref, rows)
        block = times(pick(flag, seen, own), complete(pick(flag, own, seen)))
        if first:
            prefix = pick(flag, seen, unit_rows(seen[0][0][0]))
        else:
            before = take(prefix_ref, rows)
            prefix = pick(flag, times(seen, complete(before)), before)
        give(refs[0], rows, block)
        if last:
            after = times(prefix, complete(take(lower_ref, rows)))
            give(refs[1], rows, pick(odd, after, prefix))
            give(refs[2], rows, block)
            give(refs[2], rows, pick(odd, prefix, after), 12 * half * planes)
        else:
            give(refs[1], rows, prefix)


def close(flag, block, prefix, seen):
    poly = times(pick(flag, seen, block), complete(pick(flag, block, seen)))
    return poly, pick(flag, times(seen, complete(prefix)), prefix)


def edge_kernel(planes, half, step, block_ref, prefix_ref, pair_ref, seen_ref, raw_ref, here_ref, side_ref):
    flag = bit_of(step) == 1
    rows_of = 12 * half
    for index, rows in enumerate(edge_groups(planes, half)):
        poly, prefix = close(flag, take(block_ref, rows), take(prefix_ref, rows), take(seen_ref, rows))
        partner = take(pair_ref, rows, rows_of * planes)
        partner = pick(flag, times(take(seen_ref, rows), complete(partner)), partner)
        row = lambda k: pl.ds(k * half + index, 1)
        for ref, gauge in ((here_ref, prefix), (side_ref, partner)):
            give(ref, row, poly)
            give(ref, row, gauge, rows_of)
    here_ref[2 * rows_of:, :] = raw_ref[...]


def prepare(planes, half, step, other, links_ref, block, prefix, seen, field_ref):
    slices = links_ref.shape[0]
    flag = bit_of(step) == 1
    own = bit_of(0)
    for local, rows in enumerate(groups(planes, half)):
        at = lane_block((1 - own if other else own) * half + local)
        poly, gauge = close(flag, block(rows), prefix(rows), seen(rows))
        for t in range(slices + 1):
            if 0 < t < slices:
                gauge = times(gauge, matrix_at(lambda k: links_ref[t - 1, 3, k, :, at], 3))

            def store(k, v):
                field_ref[local, 18 * t + k] = v

            put(store, complete(gauge if t < slices else poly))


def prepare_edge(half, slices, blocks, other, edge_ref, raw_ref, out_ref):
    rows_of = 12 * half
    own = bit_of(0)
    start = (1 - own if other else own) * half
    rows = lambda k: pl.ds(k * half, half)
    poly, gauge = take(edge_ref, rows), take(edge_ref, rows, rows_of)
    for t in range(slices + 1):
        if 0 < t < slices:
            base = 2 * rows_of + 12 * blocks * (t - 1)
            link = matrix_at(lambda k: raw_ref[pl.ds(base + k * blocks + start, half), :], 2)
            gauge = times(gauge, complete(link))

        def store(k, v):
            out_ref[pl.ds((18 * t + k) * half, half), :] = v

        put(store, complete(gauge if t < slices else poly))


def shifted(load, direction, r, edge):
    value = load(r)
    lane = lax.broadcasted_iota(jnp.int32, value.shape, 1)
    if direction == 0:
        row = lax.broadcasted_iota(jnp.int32, value.shape, 0)
        mixed = jnp.where(row == 0, jnp.broadcast_to(edge(r), value.shape), value)
        return pltpu.roll(mixed, value.shape[0] - 1, 0)
    if direction == 1:
        mixed = jnp.where(lane < LZ, load(r + 1), value)
        return pltpu.roll(mixed, LANES - LZ, 1)
    ahead = pltpu.roll(value, LANES - 1, 1)
    around = pltpu.roll(value, LZ - 1, 1)
    return jnp.where(lax.rem(lane, LZ) == LZ - 1, around, ahead)


def outputs(half, jobs, links_ref, fields, edges, out_ref, trace_ref, done):
    slices, cells = links_ref.shape[0], links_ref.shape[-1]
    blocks = cells // LANES
    own = bit_of(0)

    def field(r, k):
        r = r % blocks
        return fields[r // half][r % half, k]

    def edge(r, k):
        at = k * half + r % half
        return edges[r // half][at:at + 1, :]

    for job, (r, direction) in enumerate(jobs):
        at = lane_block(lax.rem(own * half + r, blocks))

        def neighbour(base):
            def one(k):
                return shifted(lambda q: field(q, base + k), direction, r, lambda q: edge(q, base + k))

            return matrix_at(one, 3)

        poly = matrix_at(lambda k: field(r, 18 * slices + k), 3)
        poly_next = neighbour(18 * slices)
        for t in range(slices):
            link = matrix_at(lambda k: links_ref[t, direction, k, :, at], 3)
            gauge = matrix_at(lambda k: field(r, 18 * t + k), 3)[:2]
            moved = complete(times_dagger(times(gauge, link), neighbour(18 * t)))

            def store(k, v):
                out_ref[job, t, k] = v

            put(store, moved)
            around = complete(times_dagger(times_dagger(moved[:2], poly_next), moved))
            trace_ref[job, t] = trace_of_product(poly, around)
        done(job)


def copies(half, jobs, out_ref, trace_ref, spatial_ref, correlator_ref, sem, job):
    r, direction = jobs[job]
    at = lane_block(lax.rem(bit_of(0) * half + r, 2 * half))
    return (
        pltpu.make_async_copy(out_ref.at[job], spatial_ref.at[:, direction, :, :, at], sem.at[job, 0]),
        pltpu.make_async_copy(trace_ref.at[job], correlator_ref.at[:, direction, :, at], sem.at[job, 1]),
    )


def jobs_of(half, stage):
    early = [(r, 2) for r in range(half)] + [(r, 1) for r in range(half - 1)]
    late = [(half - 1, 1)] + [(r, d) for r in range(half, 2 * half) for d in (1, 2)]
    return (early, late, [(r, 0) for r in range(2 * half)])[stage]


def early_kernel(planes, half, step, links_ref, block_ref, prefix_ref, seen_ref, field_ref, out_ref, trace_ref):
    prepare(planes, half, step, False, links_ref, lambda g: take(block_ref, g),
            lambda g: take(prefix_ref, g), lambda g: take(seen_ref, g), field_ref)
    outputs(half, jobs_of(half, 0), links_ref, [field_ref, field_ref], None, out_ref, trace_ref, lambda job: None)


def late_kernel(planes, half, step, links_ref, pair_ref, seen_ref, field_own, field_ref, out_ref, trace_ref):
    size = 12 * half * planes
    prepare(planes, half, step, True, links_ref, lambda g: take(pair_ref, g),
            lambda g: take(pair_ref, g, size), lambda g: take(seen_ref, g), field_ref)
    outputs(half, jobs_of(half, 1), links_ref, [field_own, field_ref], None, out_ref, trace_ref, lambda job: None)


def last_kernel(half, links_ref, here_ref, side_ref, field_own, field_other, out_early, trace_early,
                out_late, trace_late, spatial_ref, correlator_ref, edge_own, edge_other, out_ref, trace_ref,
                sem_early, sem_late, sem):
    slices, blocks = links_ref.shape[0], links_ref.shape[-1] // LANES
    made = []
    for stage, refs in enumerate(((out_early, trace_early, sem_early), (out_late, trace_late, sem_late),
                                  (out_ref, trace_ref, sem))):
        out, trace, flags = refs
        jobs = jobs_of(half, stage)
        made.append([copies(half, jobs, out, trace, spatial_ref, correlator_ref, flags, j) for j in range(len(jobs))])
    for pairs in made[:2]:
        for pair in pairs:
            for copy in pair:
                copy.start()
    prepare_edge(half, slices, blocks, False, here_ref, here_ref, edge_own)
    prepare_edge(half, slices, blocks, True, side_ref, here_ref, edge_other)

    def done(job):
        for copy in made[2][job]:
            copy.start()

    outputs(half, jobs_of(half, 2), links_ref, [field_own, field_other], [edge_own, edge_other],
            out_ref, trace_ref, done)
    for pairs in made:
        for pair in pairs:
            for copy in pair:
                copy.wait()


def in_vmem(count):
    return [pl.BlockSpec(memory_space=pltpu.VMEM)] * count


def anywhere(count):
    return [pl.BlockSpec(memory_space=pl.ANY)] * count


def cost(flops, size):
    return pl.CostEstimate(flops=flops, bytes_accessed=size, transcendentals=0)


def room(mib):
    return pltpu.CompilerParams(vmem_limit_bytes=mib << 20)


def on_device(links):
    slices, _, _, planes, cells = links.shape
    times_ta, parts_gx = lax.axis_size("ta"), lax.axis_size("gx")
    depth = times_ta.bit_length() - 1
    blocks = cells // LANES
    half = blocks // 2
    if times_ta != 1 << depth or depth < 3 or blocks % 2:
        raise ValueError("unsupported sizes")
    f32 = jnp.float32
    shape = lambda *s: jax.ShapeDtypeStruct(s, f32)
    sites = planes * cells
    size = 12 * half * planes
    raw_rows = 12 * blocks * (slices - 1)

    def across(x, step):
        return lax.ppermute(x, "ta", [(i, i ^ (1 << step)) for i in range(times_ta)])

    def product(which, width, *more):
        return pl.pallas_call(
            functools.partial(block_kernel, half, which),
            out_shape=(shape(size, LANES),) + more,
            in_specs=anywhere(1),
            out_specs=tuple(in_vmem(1 + len(more))),
            scratch_shapes=[pltpu.VMEM((slices, 18, planes, width), f32), pltpu.SemaphoreType.DMA],
            cost_estimate=cost(200 * sites, 90 * sites),
            compiler_params=room(8),
            name="block_product",
        )(pltpu.with_memory_space_constraint(links, pltpu.HBM))

    send, = product(1, half * LANES)
    seen = across(send, 0)
    keep, raw = product(0, cells, shape(max(raw_rows, 8), LANES))
    block, lower = pl.pallas_call(
        functools.partial(pair_kernel, planes, half),
        out_shape=(shape(size, LANES), shape(size, LANES)),
        in_specs=in_vmem(2),
        out_specs=tuple(in_vmem(2)),
        cost_estimate=cost(100 * sites, 50 * sites),
        compiler_params=room(8),
        name="pair",
    )(keep, seen)

    prefix = None
    for step in range(1, depth - 1):
        first, last = step == 1, step == depth - 2
        seen = across(block, step)
        operands = [block, seen] + ([] if first else [prefix]) + ([lower] if last else [])
        outs = [shape(size, LANES)] * 2 + ([shape(2 * size, LANES)] if last else [])
        block, prefix, *pair = pl.pallas_call(
            functools.partial(combine_kernel, planes, half, step, first, last),
            out_shape=tuple(outs),
            in_specs=in_vmem(len(operands)),
            out_specs=tuple(in_vmem(len(outs))),
            cost_estimate=cost(200 * sites, 100 * sites),
            compiler_params=room(8),
            name="combine",
        )(*operands)

    step = depth - 1
    seen = across(block, step)
    pair = pair[0]
    pair_back = across(pair, 0)
    seen_back = across(seen, 0)

    here, side = pl.pallas_call(
        functools.partial(edge_kernel, planes, half, step),
        out_shape=(shape(24 * half + max(raw_rows, 8), LANES), shape(24 * half, LANES)),
        in_specs=in_vmem(5),
        out_specs=tuple(in_vmem(2)),
        cost_estimate=cost(20 * sites, 10 * sites),
        compiler_params=room(8),
        name="edge",
    )(block, prefix, pair, seen, raw)
    here = lax.ppermute(here, "gx", [(i, (i - 1) % parts_gx) for i in range(parts_gx)])
    side = lax.ppermute(
        side, ("ta", "gx"),
        [(i * parts_gx + j, (i ^ 1) * parts_gx + (j - 1) % parts_gx)
         for i in range(times_ta) for j in range(parts_gx)],
    )

    def results(count):
        return [(count, slices, 18, planes, LANES), (count, slices, planes, LANES)]

    counts = [len(jobs_of(half, stage)) for stage in range(3)]
    field_shape = (half, 18 * (slices + 1), planes, LANES)
    field_own, out_early, trace_early = pl.pallas_call(
        functools.partial(early_kernel, planes, half, step),
        out_shape=tuple(shape(*s) for s in [field_shape] + results(counts[0])),
        in_specs=in_vmem(4),
        out_specs=tuple(in_vmem(3)),
        cost_estimate=cost(1200 * sites, 400 * sites),
        compiler_params=room(8),
        name="early",
    )(links, block, prefix, seen)
    field_other, out_late, trace_late = pl.pallas_call(
        functools.partial(late_kernel, planes, half, step),
        out_shape=tuple(shape(*s) for s in [field_shape] + results(counts[1])),
        in_specs=in_vmem(4),
        out_specs=tuple(in_vmem(3)),
        cost_estimate=cost(2000 * sites, 600 * sites),
        compiler_params=room(8),
        name="late",
    )(links, pair_back, seen_back, field_own)
    edge_shape = (18 * (slices + 1) * half, LANES)
    return pl.pallas_call(
        functools.partial(last_kernel, half),
        out_shape=(shape(slices, 3, 18, planes, cells), shape(slices, 3, planes, cells)),
        in_specs=in_vmem(9),
        out_specs=tuple(anywhere(2)),
        scratch_shapes=[pltpu.VMEM(s, f32) for s in [edge_shape, edge_shape] + results(counts[2])]
        + [pltpu.SemaphoreType.DMA((count, 2)) for count in counts],
        cost_estimate=cost(1500 * sites, 600 * sites),
        compiler_params=room(12),
        name="last",
    )(links, here, side, field_own, field_other, out_early, trace_early, out_late, trace_late)


def solution(mesh):
    in_specs = (P("ta", None, None, "gx", None),)
    out_specs = (P("ta", None, None, "gx", None), P("ta", None, "gx", None))
    return jax.shard_map(on_device, mesh=mesh, in_specs=in_specs, out_specs=out_specs, check_vma=False)
```

```python
import functools

import jax
import jax.numpy as jnp
from jax import lax
from jax.experimental import pallas as pl
from jax.experimental.pallas import tpu as pltpu
from jax.sharding import PartitionSpec as P


LZ = 32
LANES = 128


def total(terms):
    result = terms[0]
    for term in terms[1:]:
        result = result + term
    return result


def real_dot(left, right):
    return total([a * b for a, b in zip(left, right)])


def triples(rows, sign):
    return [([v[0] for v in row], [v[1] for v in row],
             [v[0] + v[1] if sign > 0 else v[0] - v[1] for v in row]) for row in rows]


def times(rows, matrix):
    columns = triples([[matrix[k][j] for k in range(3)] for j in range(3)], 1)
    result = []
    for left in triples(rows, 1):
        line = []
        for right in columns:
            a, b, c = (real_dot(x, y) for x, y in zip(left, right))
            line.append((a - b, c - a - b))
        result.append(line)
    return result


def times_dagger(rows, matrix):
    others = triples(matrix, -1)
    result = []
    for left in triples(rows, 1):
        line = []
        for right in others:
            a, b, c = (real_dot(x, y) for x, y in zip(left, right))
            line.append((a + b, c - a + b))
        result.append(line)
    return result


def complete(rows):
    first, second = rows[0], rows[1]
    third = []
    for j in range(3):
        a, b = (j + 1) % 3, (j + 2) % 3
        ar, ai = first[a]
        br, bi = second[b]
        cr, ci = first[b]
        dr, di = second[a]
        third.append((ar * br - ai * bi - cr * dr + ci * di, cr * di + ci * dr - ar * bi - ai * br))
    return [first, second, third]


def pick(flag, yes, no):
    return [
        [(jnp.where(flag, y[0], n[0]), jnp.where(flag, y[1], n[1])) for y, n in zip(yr, nr)]
        for yr, nr in zip(yes, no)
    ]


def unit_rows(like):
    one, zero = jnp.ones_like(like), jnp.zeros_like(like)
    return [[(one if i == j else zero, zero) for j in range(3)] for i in range(2)]


def trace_of_product(left, right):
    reals = total([left[i][j][0] * right[j][i][0] for i in range(3) for j in range(3)])
    return reals - total([left[i][j][1] * right[j][i][1] for i in range(3) for j in range(3)])


def matrix_at(at, rows):
    return [[(at(i * 3 + j), at((rows + i) * 3 + j)) for j in range(3)] for i in range(rows)]


def put(at, matrix):
    rows = len(matrix)
    for i in range(rows):
        for j in range(3):
            at(i * 3 + j, matrix[i][j][0])
            at((rows + i) * 3 + j, matrix[i][j][1])


def groups(planes, half):
    return [lambda k, block=block: pl.ds((k * half + block) * planes, planes) for block in range(half)]


def edge_groups(planes, half):
    return [lambda k, block=block: pl.ds((k * half + block) * planes, 1) for block in range(half)]


def take(ref, rows, base=0):
    return matrix_at(lambda k: ref[pl.ds(rows(k).start + base, rows(k).size), :], 2)


def give(ref, rows, matrix, base=0):
    def at(k, value):
        ref[pl.ds(rows(k).start + base, rows(k).size), :] = value

    put(at, matrix)


def bit_of(step):
    return lax.rem(lax.axis_index("ta") // (1 << step), 2)


def lane_block(c):
    return pl.ds(pl.multiple_of(c * LANES, LANES), LANES)


def block_kernel(half, which, whole_ref, block_ref, *rest):
    links_ref, sem = rest[-2:]
    slices, _, planes, cells = links_ref.shape
    blocks = whole_ref.shape[-1] // LANES
    own = bit_of(0)
    start = (own if which == 0 else 1 - own) * half if which else 0
    at = pl.ds(pl.multiple_of(start * LANES, LANES), cells)
    copy = pltpu.make_async_copy(whole_ref.at[:, 3, :, :, at], links_ref, sem)
    copy.start()
    copy.wait()
    for block in range(half):
        at = lane_block(block if which else own * half + block)
        link = lambda t: matrix_at(lambda k: links_ref[t, k, :, at], 3)
        rows = link(0)[:2]
        for t in range(1, slices):
            rows = times(rows, link(t))
        give(block_ref, groups(planes, half)[block], rows)
    if which == 0:
        for t in range(slices - 1):
            for c in range(blocks):
                def edge(k, value):
                    row = (12 * t + k) * blocks + c
                    rest[0][row:row + 1, :] = value[:1]

                put(edge, matrix_at(lambda k: links_ref[t, k, :, c * LANES:(c + 1) * LANES], 3)[:2])


def pair_kernel(planes, half, keep_ref, seen_ref, block_ref, lower_ref):
    upper = bit_of(0) == 1
    for rows in groups(planes, half):
        own, seen = take(keep_ref, rows), take(seen_ref, rows)
        low, high = pick(upper, seen, own), pick(upper, own, seen)
        give(block_ref, rows, times(low, complete(high)))
        give(lower_ref, rows, low)


def combine_kernel(planes, half, step, first, last, *refs):
    refs = list(refs)
    block_ref, seen_ref = refs.pop(0), refs.pop(0)
    prefix_ref = None if first else refs.pop(0)
    lower_ref = refs.pop(0) if last else None
    flag = bit_of(step) == 1
    odd = bit_of(0) == 1
    for rows in groups(planes, half):
        own, seen = take(block_ref, rows), take(seen_ref, rows)
        block = times(pick(flag, seen, own), complete(pick(flag, own, seen)))
        if first:
            prefix = pick(flag, seen, unit_rows(seen[0][0][0]))
        else:
            before = take(prefix_ref, rows)
            prefix = pick(flag, times(seen, complete(before)), before)
        give(refs[0], rows, block)
        if last:
            after = times(prefix, complete(take(lower_ref, rows)))
            give(refs[1], rows, pick(odd, after, prefix))
            give(refs[2], rows, block)
            give(refs[2], rows, pick(odd, prefix, after), 12 * half * planes)
        else:
            give(refs[1], rows, prefix)


def close(flag, block, prefix, seen):
    poly = times(pick(flag, seen, block), complete(pick(flag, block, seen)))
    return poly, pick(flag, times(seen, complete(prefix)), prefix)


def edge_kernel(planes, half, step, block_ref, prefix_ref, pair_ref, seen_ref, raw_ref, here_ref, side_ref):
    flag = bit_of(step) == 1
    rows_of = 12 * half
    for index, rows in enumerate(edge_groups(planes, half)):
        poly, prefix = close(flag, take(block_ref, rows), take(prefix_ref, rows), take(seen_ref, rows))
        partner = take(pair_ref, rows, rows_of * planes)
        partner = pick(flag, times(take(seen_ref, rows), complete(partner)), partner)
        row = lambda k: pl.ds(k * half + index, 1)
        for ref, gauge in ((here_ref, prefix), (side_ref, partner)):
            give(ref, row, poly)
            give(ref, row, gauge, rows_of)
    here_ref[2 * rows_of:, :] = raw_ref[...]


def prepare(planes, half, step, other, links_ref, block, prefix, seen, field_ref):
    slices = links_ref.shape[0]
    flag = bit_of(step) == 1
    own = bit_of(0)
    for local, rows in enumerate(groups(planes, half)):
        at = lane_block((1 - own if other else own) * half + local)
        poly, gauge = close(flag, block(rows), prefix(rows), seen(rows))
        for t in range(slices + 1):
            if 0 < t < slices:
                gauge = times(gauge, matrix_at(lambda k: links_ref[t - 1, 3, k, :, at], 3))

            def store(k, v):
                field_ref[local, 18 * t + k] = v

            put(store, complete(gauge if t < slices else poly))


def prepare_edge(half, slices, blocks, other, edge_ref, raw_ref, out_ref):
    rows_of = 12 * half
    own = bit_of(0)
    start = (1 - own if other else own) * half
    rows = lambda k: pl.ds(k * half, half)
    poly, gauge = take(edge_ref, rows), take(edge_ref, rows, rows_of)
    for t in range(slices + 1):
        if 0 < t < slices:
            base = 2 * rows_of + 12 * blocks * (t - 1)
            link = matrix_at(lambda k: raw_ref[pl.ds(base + k * blocks + start, half), :], 2)
            gauge = times(gauge, complete(link))

        def store(k, v):
            out_ref[pl.ds((18 * t + k) * half, half), :] = v

        put(store, complete(gauge if t < slices else poly))


def shifted(load, direction, r, edge):
    value = load(r)
    lane = lax.broadcasted_iota(jnp.int32, value.shape, 1)
    if direction == 0:
        row = lax.broadcasted_iota(jnp.int32, value.shape, 0)
        mixed = jnp.where(row == 0, jnp.broadcast_to(edge(r), value.shape), value)
        return pltpu.roll(mixed, value.shape[0] - 1, 0)
    if direction == 1:
        mixed = jnp.where(lane < LZ, load(r + 1), value)
        return pltpu.roll(mixed, LANES - LZ, 1)
    ahead = pltpu.roll(value, LANES - 1, 1)
    around = pltpu.roll(value, LZ - 1, 1)
    return jnp.where(lax.rem(lane, LZ) == LZ - 1, around, ahead)


def outputs(half, jobs, links_ref, fields, edges, out_ref, trace_ref, done):
    slices, cells = links_ref.shape[0], links_ref.shape[-1]
    blocks = cells // LANES
    own = bit_of(0)

    def field(r, k):
        r = r % blocks
        return fields[r // half][r % half, k]

    def edge(r, k):
        at = k * half + r % half
        return edges[r // half][at:at + 1, :]

    for job, (r, direction) in enumerate(jobs):
        at = lane_block(lax.rem(own * half + r, blocks))

        def neighbour(base):
            def one(k):
                return shifted(lambda q: field(q, base + k), direction, r, lambda q: edge(q, base + k))

            return matrix_at(one, 3)

        poly = matrix_at(lambda k: field(r, 18 * slices + k), 3)
        poly_next = neighbour(18 * slices)
        for t in range(slices):
            link = matrix_at(lambda k: links_ref[t, direction, k, :, at], 3)
            gauge = matrix_at(lambda k: field(r, 18 * t + k), 3)[:2]
            moved = complete(times_dagger(times(gauge, link), neighbour(18 * t)))

            def store(k, v):
                out_ref[job, t, k] = v

            put(store, moved)
            around = complete(times_dagger(times_dagger(moved[:2], poly_next), moved))
            trace_ref[job, t] = trace_of_product(poly, around)
        done(job)


def lanes_of(half, r):
    return lane_block(lax.rem(bit_of(0) * half + r, 2 * half))


def jobs_of(half, stage):
    early = [(r, 2) for r in range(half)] + [(r, 1) for r in range(half - 1)]
    late = [(half - 1, 1)] + [(r, d) for r in range(half, 2 * half) for d in (1, 2)]
    return (early, late, [(r, 0) for r in range(2 * half)])[stage]


def early_kernel(planes, half, step, links_ref, block_ref, prefix_ref, seen_ref, field_ref, out_ref, trace_ref):
    prepare(planes, half, step, False, links_ref, lambda g: take(block_ref, g),
            lambda g: take(prefix_ref, g), lambda g: take(seen_ref, g), field_ref)
    outputs(half, jobs_of(half, 0), links_ref, [field_ref, field_ref], None, out_ref, trace_ref, lambda job: None)


def late_kernel(planes, half, step, links_ref, pair_ref, seen_ref, field_own, field_ref, out_ref, trace_ref):
    size = 12 * half * planes
    prepare(planes, half, step, True, links_ref, lambda g: take(pair_ref, g),
            lambda g: take(pair_ref, g, size), lambda g: take(seen_ref, g), field_ref)
    outputs(half, jobs_of(half, 1), links_ref, [field_own, field_ref], None, out_ref, trace_ref, lambda job: None)


def last_kernel(half, links_ref, here_ref, side_ref, field_own, field_other, out_early, trace_early,
                out_late, trace_late, spatial_ref, correlator_ref, edge_own, edge_other, out_ref, trace_ref,
                trace_all, sem_early, sem_late, sem, sem_all):
    slices, blocks = links_ref.shape[0], links_ref.shape[-1] // LANES
    started = []

    def write(out, flags, job, r, direction):
        target = spatial_ref.at[:, direction, :, :, lanes_of(half, r)]
        copy = pltpu.make_async_copy(out.at[job], target, flags.at[job])
        copy.start()
        started.append(copy)

    def collect(trace, job, r, direction):
        trace_all[:, direction, :, lanes_of(half, r)] = trace[job]

    for stage, (out, trace, flags) in enumerate(((out_early, trace_early, sem_early), (out_late, trace_late, sem_late))):
        for job, (r, direction) in enumerate(jobs_of(half, stage)):
            write(out, flags, job, r, direction)
            collect(trace, job, r, direction)
    prepare_edge(half, slices, blocks, False, here_ref, here_ref, edge_own)
    prepare_edge(half, slices, blocks, True, side_ref, here_ref, edge_other)
    jobs = jobs_of(half, 2)

    def done(job):
        write(out_ref, sem, job, *jobs[job])
        collect(trace_ref, job, *jobs[job])

    outputs(half, jobs, links_ref, [field_own, field_other], [edge_own, edge_other], out_ref, trace_ref, done)
    copy = pltpu.make_async_copy(trace_all, correlator_ref, sem_all)
    copy.start()
    for other in started + [copy]:
        other.wait()


def in_vmem(count):
    return [pl.BlockSpec(memory_space=pltpu.VMEM)] * count


def anywhere(count):
    return [pl.BlockSpec(memory_space=pl.ANY)] * count


def cost(flops, size):
    return pl.CostEstimate(flops=flops, bytes_accessed=size, transcendentals=0)


def room(mib):
    return pltpu.CompilerParams(vmem_limit_bytes=mib << 20)


def on_device(links):
    slices, _, _, planes, cells = links.shape
    times_ta, parts_gx = lax.axis_size("ta"), lax.axis_size("gx")
    depth = times_ta.bit_length() - 1
    blocks = cells // LANES
    half = blocks // 2
    if times_ta != 1 << depth or depth < 3 or blocks % 2:
        raise ValueError("unsupported sizes")
    f32 = jnp.float32
    shape = lambda *s: jax.ShapeDtypeStruct(s, f32)
    sites = planes * cells
    size = 12 * half * planes
    raw_rows = 12 * blocks * (slices - 1)

    def across(x, step):
        return lax.ppermute(x, "ta", [(i, i ^ (1 << step)) for i in range(times_ta)])

    def product(which, width, *more):
        return pl.pallas_call(
            functools.partial(block_kernel, half, which),
            out_shape=(shape(size, LANES),) + more,
            in_specs=anywhere(1),
            out_specs=tuple(in_vmem(1 + len(more))),
            scratch_shapes=[pltpu.VMEM((slices, 18, planes, width), f32), pltpu.SemaphoreType.DMA],
            cost_estimate=cost(200 * sites, 90 * sites),
            compiler_params=room(8),
            name="block_product",
        )(pltpu.with_memory_space_constraint(links, pltpu.HBM))

    send, = product(1, half * LANES)
    seen = across(send, 0)
    keep, raw = product(0, cells, shape(max(raw_rows, 8), LANES))
    block, lower = pl.pallas_call(
        functools.partial(pair_kernel, planes, half),
        out_shape=(shape(size, LANES), shape(size, LANES)),
        in_specs=in_vmem(2),
        out_specs=tuple(in_vmem(2)),
        cost_estimate=cost(100 * sites, 50 * sites),
        compiler_params=room(8),
        name="pair",
    )(keep, seen)

    prefix = None
    for step in range(1, depth - 1):
        first, last = step == 1, step == depth - 2
        seen = across(block, step)
        operands = [block, seen] + ([] if first else [prefix]) + ([lower] if last else [])
        outs = [shape(size, LANES)] * 2 + ([shape(2 * size, LANES)] if last else [])
        block, prefix, *pair = pl.pallas_call(
            functools.partial(combine_kernel, planes, half, step, first, last),
            out_shape=tuple(outs),
            in_specs=in_vmem(len(operands)),
            out_specs=tuple(in_vmem(len(outs))),
            cost_estimate=cost(200 * sites, 100 * sites),
            compiler_params=room(8),
            name="combine",
        )(*operands)

    step = depth - 1
    seen = across(block, step)
    pair = pair[0]
    pair_back = across(pair, 0)
    seen_back = across(seen, 0)

    here, side = pl.pallas_call(
        functools.partial(edge_kernel, planes, half, step),
        out_shape=(shape(24 * half + max(raw_rows, 8), LANES), shape(24 * half, LANES)),
        in_specs=in_vmem(5),
        out_specs=tuple(in_vmem(2)),
        cost_estimate=cost(20 * sites, 10 * sites),
        compiler_params=room(8),
        name="edge",
    )(block, prefix, pair, seen, raw)
    here = lax.ppermute(here, "gx", [(i, (i - 1) % parts_gx) for i in range(parts_gx)])
    side = lax.ppermute(
        side, ("ta", "gx"),
        [(i * parts_gx + j, (i ^ 1) * parts_gx + (j - 1) % parts_gx)
         for i in range(times_ta) for j in range(parts_gx)],
    )

    def results(count):
        return [(count, slices, 18, planes, LANES), (count, slices, planes, LANES)]

    counts = [len(jobs_of(half, stage)) for stage in range(3)]
    field_shape = (half, 18 * (slices + 1), planes, LANES)
    field_own, out_early, trace_early = pl.pallas_call(
        functools.partial(early_kernel, planes, half, step),
        out_shape=tuple(shape(*s) for s in [field_shape] + results(counts[0])),
        in_specs=in_vmem(4),
        out_specs=tuple(in_vmem(3)),
        cost_estimate=cost(1200 * sites, 400 * sites),
        compiler_params=room(8),
        name="early",
    )(links, block, prefix, seen)
    field_other, out_late, trace_late = pl.pallas_call(
        functools.partial(late_kernel, planes, half, step),
        out_shape=tuple(shape(*s) for s in [field_shape] + results(counts[1])),
        in_specs=in_vmem(4),
        out_specs=tuple(in_vmem(3)),
        cost_estimate=cost(2000 * sites, 600 * sites),
        compiler_params=room(8),
        name="late",
    )(links, pair_back, seen_back, field_own)
    edge_shape = (18 * (slices + 1) * half, LANES)
    return pl.pallas_call(
        functools.partial(last_kernel, half),
        out_shape=(shape(slices, 3, 18, planes, cells), shape(slices, 3, planes, cells)),
        in_specs=in_vmem(9),
        out_specs=tuple(anywhere(2)),
        scratch_shapes=[pltpu.VMEM(s, f32) for s in [edge_shape, edge_shape] + results(counts[2])]
        + [pltpu.VMEM((slices, 3, planes, cells), f32)]
        + [pltpu.SemaphoreType.DMA((count,)) for count in counts] + [pltpu.SemaphoreType.DMA],
        cost_estimate=cost(1500 * sites, 600 * sites),
        compiler_params=room(12),
        name="last",
    )(links, here, side, field_own, field_other, out_early, trace_early, out_late, trace_late)


def solution(mesh):
    in_specs = (P("ta", None, None, "gx", None),)
    out_specs = (P("ta", None, None, "gx", None), P("ta", None, "gx", None))
    return jax.shard_map(on_device, mesh=mesh, in_specs=in_specs, out_specs=out_specs, check_vma=False)
```

```python
import functools

import jax
import jax.numpy as jnp
from jax import lax
from jax.experimental import pallas as pl
from jax.experimental.pallas import tpu as pltpu
from jax.sharding import PartitionSpec as P


LZ = 32
LANES = 128


def total(terms):
    result = terms[0]
    for term in terms[1:]:
        result = result + term
    return result


def real_dot(left, right):
    return total([a * b for a, b in zip(left, right)])


def triples(rows, sign):
    return [([v[0] for v in row], [v[1] for v in row],
             [v[0] + v[1] if sign > 0 else v[0] - v[1] for v in row]) for row in rows]


def times(rows, matrix):
    columns = triples([[matrix[k][j] for k in range(3)] for j in range(3)], 1)
    result = []
    for left in triples(rows, 1):
        line = []
        for right in columns:
            a, b, c = (real_dot(x, y) for x, y in zip(left, right))
            line.append((a - b, c - a - b))
        result.append(line)
    return result


def times_dagger(rows, matrix):
    others = triples(matrix, -1)
    result = []
    for left in triples(rows, 1):
        line = []
        for right in others:
            a, b, c = (real_dot(x, y) for x, y in zip(left, right))
            line.append((a + b, c - a + b))
        result.append(line)
    return result


def complete(rows):
    first, second = rows[0], rows[1]
    third = []
    for j in range(3):
        a, b = (j + 1) % 3, (j + 2) % 3
        ar, ai = first[a]
        br, bi = second[b]
        cr, ci = first[b]
        dr, di = second[a]
        third.append((ar * br - ai * bi - cr * dr + ci * di, cr * di + ci * dr - ar * bi - ai * br))
    return [first, second, third]


def pick(flag, yes, no):
    return [
        [(jnp.where(flag, y[0], n[0]), jnp.where(flag, y[1], n[1])) for y, n in zip(yr, nr)]
        for yr, nr in zip(yes, no)
    ]


def unit_rows(like):
    one, zero = jnp.ones_like(like), jnp.zeros_like(like)
    return [[(one if i == j else zero, zero) for j in range(3)] for i in range(2)]


def trace_of_product(left, right):
    reals = total([left[i][j][0] * right[j][i][0] for i in range(3) for j in range(3)])
    return reals - total([left[i][j][1] * right[j][i][1] for i in range(3) for j in range(3)])


def matrix_at(at, rows):
    return [[(at(i * 3 + j), at((rows + i) * 3 + j)) for j in range(3)] for i in range(rows)]


def put(at, matrix):
    rows = len(matrix)
    for i in range(rows):
        for j in range(3):
            at(i * 3 + j, matrix[i][j][0])
            at((rows + i) * 3 + j, matrix[i][j][1])


def groups(planes, half):
    return [lambda k, block=block: pl.ds((k * half + block) * planes, planes) for block in range(half)]


def take(ref, rows, base=0):
    return matrix_at(lambda k: ref[pl.ds(rows(k).start + base, rows(k).size), :], 2)


def give(ref, rows, matrix, base=0):
    def at(k, value):
        ref[pl.ds(rows(k).start + base, rows(k).size), :] = value

    put(at, matrix)


def bit_of(step):
    return lax.rem(lax.axis_index("ta") // (1 << step), 2)


def lane_block(c):
    return pl.ds(pl.multiple_of(c * LANES, LANES), LANES)


def block_kernel(half, which, whole_ref, block_ref, *rest):
    links_ref, sem = rest[-2:]
    slices, _, planes, cells = links_ref.shape
    blocks = whole_ref.shape[-1] // LANES
    own = bit_of(0)
    start = (own if which == 0 else 1 - own) * half if which else 0
    at = pl.ds(pl.multiple_of(start * LANES, LANES), cells)
    copy = pltpu.make_async_copy(whole_ref.at[:, 3, :, :, at], links_ref, sem)
    copy.start()
    copy.wait()
    for block in range(half):
        at = lane_block(block if which else own * half + block)
        link = lambda t: matrix_at(lambda k: links_ref[t, k, :, at], 3)
        rows = link(0)[:2]
        for t in range(1, slices):
            rows = times(rows, link(t))
        give(block_ref, groups(planes, half)[block], rows)
    if which == 0:
        for t in range(slices - 1):
            for c in range(blocks):
                def edge(k, value):
                    row = (12 * t + k) * blocks + c
                    rest[0][row:row + 1, :] = value[:1]

                put(edge, matrix_at(lambda k: links_ref[t, k, :, c * LANES:(c + 1) * LANES], 3)[:2])


def pair_kernel(planes, half, keep_ref, seen_ref, block_ref, lower_ref):
    upper = bit_of(0) == 1
    for rows in groups(planes, half):
        own, seen = take(keep_ref, rows), take(seen_ref, rows)
        low, high = pick(upper, seen, own), pick(upper, own, seen)
        give(block_ref, rows, times(low, complete(high)))
        give(lower_ref, rows, low)


def combine_kernel(planes, half, step, first, last, *refs):
    refs = list(refs)
    block_ref, seen_ref = refs.pop(0), refs.pop(0)
    prefix_ref = None if first else refs.pop(0)
    lower_ref = refs.pop(0) if last else None
    flag = bit_of(step) == 1
    odd = bit_of(0) == 1
    for rows in groups(planes, half):
        own, seen = take(block_ref, rows), take(seen_ref, rows)
        block = times(pick(flag, seen, own), complete(pick(flag, own, seen)))
        if first:
            prefix = pick(flag, seen, unit_rows(seen[0][0][0]))
        else:
            before = take(prefix_ref, rows)
            prefix = pick(flag, times(seen, complete(before)), before)
        give(refs[0], rows, block)
        if last:
            after = times(prefix, complete(take(lower_ref, rows)))
            give(refs[1], rows, pick(odd, after, prefix))
            give(refs[2], rows, block)
            give(refs[2], rows, pick(odd, prefix, after), 12 * half * planes)
        else:
            give(refs[1], rows, prefix)


def close(flag, block, prefix, seen):
    poly = times(pick(flag, seen, block), complete(pick(flag, block, seen)))
    return poly, pick(flag, times(seen, complete(prefix)), prefix)


def edge_kernel(planes, half, step, block_ref, prefix_ref, pair_ref, seen_ref, raw_ref, here_ref, side_ref):
    flag = bit_of(step) == 1
    rows_of = 12 * half

    def plane(ref, base=0):
        return matrix_at(lambda k: ref[pl.ds(base + k * half * planes, half, stride=planes), :], 2)

    seen = plane(seen_ref)
    poly, prefix = close(flag, plane(block_ref), plane(prefix_ref), seen)
    partner = plane(pair_ref, rows_of * planes)
    partner = pick(flag, times(seen, complete(partner)), partner)
    rows = lambda k: pl.ds(k * half, half)
    for ref, gauge in ((here_ref, prefix), (side_ref, partner)):
        give(ref, rows, poly)
        give(ref, rows, gauge, rows_of)
    here_ref[2 * rows_of:, :] = raw_ref[...]


def prepare(planes, half, step, other, links_ref, block, prefix, seen, field_ref):
    slices = links_ref.shape[0]
    flag = bit_of(step) == 1
    own = bit_of(0)
    for local, rows in enumerate(groups(planes, half)):
        at = lane_block((1 - own if other else own) * half + local)
        poly, gauge = close(flag, block(rows), prefix(rows), seen(rows))
        for t in range(slices + 1):
            if 0 < t < slices:
                gauge = times(gauge, matrix_at(lambda k: links_ref[t - 1, 3, k, :, at], 3))

            def store(k, v):
                field_ref[local, 18 * t + k] = v

            put(store, complete(gauge if t < slices else poly))


def prepare_edge(half, slices, blocks, other, edge_ref, raw_ref, out_ref):
    rows_of = 12 * half
    own = bit_of(0)
    start = (1 - own if other else own) * half
    rows = lambda k: pl.ds(k * half, half)
    poly, gauge = take(edge_ref, rows), take(edge_ref, rows, rows_of)
    for t in range(slices + 1):
        if 0 < t < slices:
            base = 2 * rows_of + 12 * blocks * (t - 1)
            link = matrix_at(lambda k: raw_ref[pl.ds(base + k * blocks + start, half), :], 2)
            gauge = times(gauge, complete(link))

        def store(k, v):
            out_ref[pl.ds((18 * t + k) * half, half), :] = v

        put(store, complete(gauge if t < slices else poly))


def shifted(load, direction, r, edge):
    value = load(r)
    lane = lax.broadcasted_iota(jnp.int32, value.shape, 1)
    if direction == 0:
        row = lax.broadcasted_iota(jnp.int32, value.shape, 0)
        mixed = jnp.where(row == 0, jnp.broadcast_to(edge(r), value.shape), value)
        return pltpu.roll(mixed, value.shape[0] - 1, 0)
    if direction == 1:
        mixed = jnp.where(lane < LZ, load(r + 1), value)
        return pltpu.roll(mixed, LANES - LZ, 1)
    ahead = pltpu.roll(value, LANES - 1, 1)
    around = pltpu.roll(value, LZ - 1, 1)
    return jnp.where(lax.rem(lane, LZ) == LZ - 1, around, ahead)


def outputs(half, jobs, links_ref, fields, edges, out_ref, trace_ref, done):
    slices, cells = links_ref.shape[0], links_ref.shape[-1]
    blocks = cells // LANES
    own = bit_of(0)

    def field(r, k):
        r = r % blocks
        return fields[r // half][r % half, k]

    def edge(r, k):
        at = k * half + r % half
        return edges[r // half][at:at + 1, :]

    for job, (r, direction) in enumerate(jobs):
        at = lane_block(lax.rem(own * half + r, blocks))

        def neighbour(base):
            def one(k):
                return shifted(lambda q: field(q, base + k), direction, r, lambda q: edge(q, base + k))

            return matrix_at(one, 3)

        poly = matrix_at(lambda k: field(r, 18 * slices + k), 3)
        poly_next = neighbour(18 * slices)
        for t in range(slices):
            link = matrix_at(lambda k: links_ref[t, direction, k, :, at], 3)
            gauge = matrix_at(lambda k: field(r, 18 * t + k), 3)[:2]
            moved = complete(times_dagger(times(gauge, link), neighbour(18 * t)))

            def store(k, v):
                out_ref[job, t, k] = v

            put(store, moved)
            around = complete(times_dagger(times_dagger(moved[:2], poly_next), moved))
            trace_ref[job, t] = trace_of_product(poly, around)
        done(job)


def lanes_of(half, r):
    return lane_block(lax.rem(bit_of(0) * half + r, 2 * half))


def jobs_of(half, stage):
    early = [(r, 2) for r in range(half)] + [(r, 1) for r in range(half - 1)]
    late = [(half - 1, 1)] + [(r, d) for r in range(half, 2 * half) for d in (1, 2)]
    return (early, late, [(r, 0) for r in range(2 * half)])[stage]


def early_kernel(planes, half, step, links_ref, block_ref, prefix_ref, seen_ref, field_ref, out_ref, trace_ref):
    prepare(planes, half, step, False, links_ref, lambda g: take(block_ref, g),
            lambda g: take(prefix_ref, g), lambda g: take(seen_ref, g), field_ref)
    outputs(half, jobs_of(half, 0), links_ref, [field_ref, field_ref], None, out_ref, trace_ref, lambda job: None)


def late_kernel(planes, half, step, links_ref, pair_ref, seen_ref, field_own, field_ref, out_ref, trace_ref):
    size = 12 * half * planes
    prepare(planes, half, step, True, links_ref, lambda g: take(pair_ref, g),
            lambda g: take(pair_ref, g, size), lambda g: take(seen_ref, g), field_ref)
    outputs(half, jobs_of(half, 1), links_ref, [field_own, field_ref], None, out_ref, trace_ref, lambda job: None)


def last_kernel(half, links_ref, here_ref, side_ref, field_own, field_other, out_early, trace_early,
                out_late, trace_late, spatial_ref, correlator_ref, edge_own, edge_other, out_ref, trace_ref,
                trace_all, sem_early, sem_late, sem, sem_all):
    slices, blocks = links_ref.shape[0], links_ref.shape[-1] // LANES
    started = []

    def write(out, flags, job, r, direction):
        target = spatial_ref.at[:, direction, :, :, lanes_of(half, r)]
        copy = pltpu.make_async_copy(out.at[job], target, flags.at[job])
        copy.start()
        started.append(copy)

    def collect(trace, job, r, direction):
        trace_all[:, direction, :, lanes_of(half, r)] = trace[job]

    for stage, (out, trace, flags) in enumerate(((out_early, trace_early, sem_early), (out_late, trace_late, sem_late))):
        for job, (r, direction) in enumerate(jobs_of(half, stage)):
            write(out, flags, job, r, direction)
            collect(trace, job, r, direction)
    prepare_edge(half, slices, blocks, False, here_ref, here_ref, edge_own)
    prepare_edge(half, slices, blocks, True, side_ref, here_ref, edge_other)
    jobs = jobs_of(half, 2)

    def done(job):
        write(out_ref, sem, job, *jobs[job])
        collect(trace_ref, job, *jobs[job])

    outputs(half, jobs, links_ref, [field_own, field_other], [edge_own, edge_other], out_ref, trace_ref, done)
    copy = pltpu.make_async_copy(trace_all, correlator_ref, sem_all)
    copy.start()
    for other in started + [copy]:
        other.wait()


def in_vmem(count):
    return [pl.BlockSpec(memory_space=pltpu.VMEM)] * count


def anywhere(count):
    return [pl.BlockSpec(memory_space=pl.ANY)] * count


def cost(flops, size):
    return pl.CostEstimate(flops=flops, bytes_accessed=size, transcendentals=0)


def room(mib):
    return pltpu.CompilerParams(vmem_limit_bytes=mib << 20)


def on_device(links):
    slices, _, _, planes, cells = links.shape
    times_ta, parts_gx = lax.axis_size("ta"), lax.axis_size("gx")
    depth = times_ta.bit_length() - 1
    blocks = cells // LANES
    half = blocks // 2
    if times_ta != 1 << depth or depth < 3 or blocks % 2:
        raise ValueError("unsupported sizes")
    f32 = jnp.float32
    shape = lambda *s: jax.ShapeDtypeStruct(s, f32)
    sites = planes * cells
    size = 12 * half * planes
    raw_rows = 12 * blocks * (slices - 1)

    def across(x, step):
        return lax.ppermute(x, "ta", [(i, i ^ (1 << step)) for i in range(times_ta)])

    def product(which, width, *more):
        return pl.pallas_call(
            functools.partial(block_kernel, half, which),
            out_shape=(shape(size, LANES),) + more,
            in_specs=anywhere(1),
            out_specs=tuple(in_vmem(1 + len(more))),
            scratch_shapes=[pltpu.VMEM((slices, 18, planes, width), f32), pltpu.SemaphoreType.DMA],
            cost_estimate=cost(200 * sites, 90 * sites),
            compiler_params=room(8),
            name="block_product",
        )(pltpu.with_memory_space_constraint(links, pltpu.HBM))

    send, = product(1, half * LANES)
    seen = across(send, 0)
    keep, raw = product(0, cells, shape(max(raw_rows, 8), LANES))
    block, lower = pl.pallas_call(
        functools.partial(pair_kernel, planes, half),
        out_shape=(shape(size, LANES), shape(size, LANES)),
        in_specs=in_vmem(2),
        out_specs=tuple(in_vmem(2)),
        cost_estimate=cost(100 * sites, 50 * sites),
        compiler_params=room(8),
        name="pair",
    )(keep, seen)

    prefix = None
    for step in range(1, depth - 1):
        first, last = step == 1, step == depth - 2
        seen = across(block, step)
        operands = [block, seen] + ([] if first else [prefix]) + ([lower] if last else [])
        outs = [shape(size, LANES)] * 2 + ([shape(2 * size, LANES)] if last else [])
        block, prefix, *pair = pl.pallas_call(
            functools.partial(combine_kernel, planes, half, step, first, last),
            out_shape=tuple(outs),
            in_specs=in_vmem(len(operands)),
            out_specs=tuple(in_vmem(len(outs))),
            cost_estimate=cost(200 * sites, 100 * sites),
            compiler_params=room(8),
            name="combine",
        )(*operands)

    step = depth - 1
    seen = across(block, step)
    pair = pair[0]
    pair_back = across(pair, 0)
    seen_back = across(seen, 0)

    here, side = pl.pallas_call(
        functools.partial(edge_kernel, planes, half, step),
        out_shape=(shape(24 * half + max(raw_rows, 8), LANES), shape(24 * half, LANES)),
        in_specs=in_vmem(5),
        out_specs=tuple(in_vmem(2)),
        cost_estimate=cost(20 * sites, 10 * sites),
        compiler_params=room(8),
        name="edge",
    )(block, prefix, pair, seen, raw)
    here = lax.ppermute(here, "gx", [(i, (i - 1) % parts_gx) for i in range(parts_gx)])
    side = lax.ppermute(
        side, ("ta", "gx"),
        [(i * parts_gx + j, (i ^ 1) * parts_gx + (j - 1) % parts_gx)
         for i in range(times_ta) for j in range(parts_gx)],
    )

    def results(count):
        return [(count, slices, 18, planes, LANES), (count, slices, planes, LANES)]

    counts = [len(jobs_of(half, stage)) for stage in range(3)]
    field_shape = (half, 18 * (slices + 1), planes, LANES)
    field_own, out_early, trace_early = pl.pallas_call(
        functools.partial(early_kernel, planes, half, step),
        out_shape=tuple(shape(*s) for s in [field_shape] + results(counts[0])),
        in_specs=in_vmem(4),
        out_specs=tuple(in_vmem(3)),
        cost_estimate=cost(1200 * sites, 400 * sites),
        compiler_params=room(8),
        name="early",
    )(links, block, prefix, seen)
    field_other, out_late, trace_late = pl.pallas_call(
        functools.partial(late_kernel, planes, half, step),
        out_shape=tuple(shape(*s) for s in [field_shape] + results(counts[1])),
        in_specs=in_vmem(4),
        out_specs=tuple(in_vmem(3)),
        cost_estimate=cost(2000 * sites, 600 * sites),
        compiler_params=room(8),
        name="late",
    )(links, pair_back, seen_back, field_own)
    edge_shape = (18 * (slices + 1) * half, LANES)
    return pl.pallas_call(
        functools.partial(last_kernel, half),
        out_shape=(shape(slices, 3, 18, planes, cells), shape(slices, 3, planes, cells)),
        in_specs=in_vmem(9),
        out_specs=tuple(anywhere(2)),
        scratch_shapes=[pltpu.VMEM(s, f32) for s in [edge_shape, edge_shape] + results(counts[2])]
        + [pltpu.VMEM((slices, 3, planes, cells), f32)]
        + [pltpu.SemaphoreType.DMA((count,)) for count in counts] + [pltpu.SemaphoreType.DMA],
        cost_estimate=cost(1500 * sites, 600 * sites),
        compiler_params=room(12),
        name="last",
    )(links, here, side, field_own, field_other, out_early, trace_early, out_late, trace_late)


def solution(mesh):
    in_specs = (P("ta", None, None, "gx", None),)
    out_specs = (P("ta", None, None, "gx", None), P("ta", None, "gx", None))
    return jax.shard_map(on_device, mesh=mesh, in_specs=in_specs, out_specs=out_specs, check_vma=False)
```
